32 devices in a mesh: seq: 16 (over z, y, x), tensor: 2 (over core).
Axes of the slice: x: 2, y: 2, z: 4, core: 2. Of those that a mesh axis runs over, the one named last changes fastest.
Arguments:
- inputs: bfloat16 [1, 8192, 1024], P(None, 'seq'), may hold values from -6 to 6
- out_grad: bfloat16 [1, 8192, 1024], P(None, 'seq'), may hold values from -6 to 6
- mix_gain: bfloat16 [1, 1024], replicated, may hold values from 0.25 to 1.75
- in_weight: bfloat16 [1, 1024, 3, 1024], P(None, None, None, 'tensor'), may hold values from -0.1875 to 0.1875
- conv_weight: bfloat16 [1, 3, 1024], P(None, None, 'tensor'), may hold values from -3.5 to 3.5
- out_weight: bfloat16 [1, 1024, 1024], P(None, 'tensor'), may hold values from -0.1875 to 0.1875
- ffn_gain: bfloat16 [1, 1024], replicated, may hold values from 0.25 to 1.75
- gate_weight: bfloat16 [1, 1024, 4608], P(None, None, 'tensor'), may hold values from -0.1875 to 0.1875
- up_weight: bfloat16 [1, 1024, 4608], P(None, None, 'tensor'), may hold values from -0.1875 to 0.1875
- down_weight: bfloat16 [1, 4608, 1024], P(None, 'tensor'), may hold values from -0.09375 to 0.09375
Outputs:
- output: bfloat16 [1, 8192, 1024], P(None, 'seq')
- in_grad: float32 [1, 8192, 1024], P(None, 'seq')
- mix_gain_grad: float32 [1, 1024], P(None, 'seq')
- in_weight_grad: float32 [1, 1024, 3, 1024], P(None, 'seq', None, 'tensor')
- conv_weight_grad: float32 [1, 3, 1024], P(None, None, ('tensor', 'seq'))
- out_weight_grad: float32 [1, 1024, 1024], P(None, ('tensor', 'seq'))
- ffn_gain_grad: float32 [1, 1024], P(None, 'seq')
- gate_weight_grad: float32 [1, 1024, 4608], P(None, 'seq', 'tensor')
- up_weight_grad: float32 [1, 1024, 4608], P(None, 'seq', 'tensor')
- down_weight_grad: float32 [1, 4608, 1024], P(None, ('tensor', 'seq'))
The draws below stay inside these ranges and needn't reach their ends.
All inputs are finite; a program needn't handle non-finite values.
Results may differ from the reference program's by a relative error of at most 0.011.
Values may be sent and summed in bfloat16 or wider, within the bound.
A program may use at most 192 MiB of HBM per device.

```python
import jax
import jax.numpy as jnp
from jax import lax

D = 1024
FF = 4608
CONV = 3
LAYERS = 1
LENGTH = 8192
SEQS = 1


def raised(drawn, stream_key, source, target, parts, factor):
    def block_of(dim):
        return (jnp.arange(drawn.shape[dim]) // (drawn.shape[dim] // parts)).reshape((-1,) + (1,) * (drawn.ndim - 1 - dim))

    near = jax.random.permutation(stream_key, parts)[block_of(target)]
    far = (block_of(target) + parts // 2) % parts
    return jnp.where((block_of(source) == near) | (block_of(source) == far), factor * drawn, drawn)


def shard_levels(rng, shape, cuts, low, largest):
    def one(position, blocks):
        draws = jax.random.uniform(jax.random.fold_in(jax.random.fold_in(rng, 6), position), (blocks,), jnp.float32, low / len(cuts), largest / len(cuts))
        return jnp.repeat(jnp.exp(draws), shape[position] // blocks).reshape((-1,) + (1,) * (len(shape) - position - 1))

    factor_of = one(*cuts[0])
    for cut in cuts[1:]:
        factor_of = factor_of * one(*cut)
    return factor_of


def gaussian(rng, dims, spread, reach, shards=(), held_as=jnp.bfloat16):
    array = spread * jax.random.normal(rng, dims, jnp.float32)
    if shards:
        array = array * shard_levels(rng, dims, shards, -0.22, 0.18)
    return jnp.clip(array, -reach, reach).astype(held_as)


def gaussian_with(own_key, extent, width, limit, cuts, heavy, kind=jnp.bfloat16):
    entries = width * jax.random.normal(own_key, extent, jnp.float32)
    if cuts:
        entries = entries * shard_levels(own_key, extent, cuts, -0.22, 0.18)
    return jnp.clip(raised(entries, jax.random.fold_in(own_key, 3), *heavy), -limit, limit).astype(kind)


def setup_inputs(seed: int = 0) -> dict:
    seeds = jax.random.split(jax.random.key(seed), 11)
    inputs = gaussian_with(seeds[0], (SEQS, LENGTH, D), 1.0, 6.0, ((1, 16),), (1, 2, 16, 2.0))
    out_grad = gaussian(seeds[1], (SEQS, LENGTH, D), 1.0, 6.0, ((1, 16),))
    mix_gain = jnp.clip(1.0 + 0.15 * jax.random.normal(seeds[2], (LAYERS, D), jnp.float32), 0.25, 1.75).astype(jnp.bfloat16)
    in_weight = gaussian(seeds[3], (LAYERS, D, 3, D), D ** -0.5, 0.1875, ((3, 2),))
    conv_weight = gaussian(seeds[4], (LAYERS, CONV, D), CONV ** -0.5, 3.5, ((2, 2),))
    out_weight = gaussian(seeds[5], (LAYERS, D, D), D ** -0.5, 0.1875, ((1, 2),))
    ffn_gain = jnp.clip(1.0 + 0.15 * jax.random.normal(seeds[6], (LAYERS, D), jnp.float32), 0.25, 1.75).astype(jnp.bfloat16)
    gate_weight = gaussian(seeds[7], (LAYERS, D, FF), D ** -0.5, 0.1875, ((2, 2),))
    up_weight = gaussian(seeds[8], (LAYERS, D, FF), D ** -0.5, 0.1875, ((2, 2),))
    down_weight = gaussian(seeds[9], (LAYERS, FF, D), FF ** -0.5, 0.09375, ((1, 2),))
    return dict(inputs=inputs, out_grad=out_grad, mix_gain=mix_gain, in_weight=in_weight, conv_weight=conv_weight, out_weight=out_weight, ffn_gain=ffn_gain, gate_weight=gate_weight, up_weight=up_weight, down_weight=down_weight)


@jax.custom_vjp
def low(v):
    return lax.optimization_barrier(v.astype(jnp.bfloat16)).astype(jnp.float32)

@jax.custom_vjp
def low_back(v):
    return v

def low_keep(v):
    return (low(v), None)

def low_pass(kept, grad):
    return (grad,)

def back_keep(v):
    return (v, None)

def back_low(kept, grad):
    return (low(grad),)
low.defvjp(low_keep, low_pass)
low_back.defvjp(back_keep, back_low)
EPSILON = 1e-05
HIGHEST = lax.Precision.HIGHEST

def inverse_rms(stream):
    return lax.rsqrt(lax.optimization_barrier(jnp.mean(stream * stream, axis=-1, keepdims=True)) + EPSILON)

def block_forward(stream, weights):
    gain_mix, weight_in, weight_conv, weight_out, gain_ffn, weight_gate, weight_up, weight_down = weights
    token_count = stream.shape[0]
    model_width = stream.shape[1]
    normed_mix = low(stream * inverse_rms(stream) * gain_mix)
    projected = low_back(jnp.dot(normed_mix, weight_in.reshape(model_width, 3 * model_width), precision=HIGHEST))
    projected = projected.reshape(token_count, 3, model_width)
    gated_in = projected[:, 0] * projected[:, 2]
    padded = jnp.pad(gated_in, ((2, 0), (0, 0)))
    convolved = weight_conv[0] * padded[:-2] + weight_conv[1] * padded[1:-1] + weight_conv[2] * padded[2:]
    mixed_out = low(projected[:, 1] * convolved)
    middle = stream + low_back(jnp.dot(mixed_out, weight_out, precision=HIGHEST))
    normed_ffn = low(middle * inverse_rms(middle) * gain_ffn)
    gate_pre = low_back(jnp.dot(normed_ffn, weight_gate, precision=HIGHEST))
    up_pre = low_back(jnp.dot(normed_ffn, weight_up, precision=HIGHEST))
    activated = low(jax.nn.silu(gate_pre) * up_pre)
    return middle + low_back(jnp.dot(activated, weight_down, precision=HIGHEST))

def network(stream, params_all):
    for number in range(LAYERS):
        stream = block_forward(stream, tuple((weight[number] for weight in params_all)))
    return stream

def reference(inputs, out_grad, mix_gain, in_weight, conv_weight, out_weight, ffn_gain, gate_weight, up_weight, down_weight):
    params_all = tuple((weight.astype(jnp.float32) for weight in (mix_gain, in_weight, conv_weight, out_weight, ffn_gain, gate_weight, up_weight, down_weight)))
    starting = tuple((jnp.zeros(weight.shape, jnp.float32) for weight in params_all))

    def one_sequence(totals, sequence_pair):
        sequence_in, sequence_grad = sequence_pair
        result, pullback = jax.vjp(network, sequence_in.astype(jnp.float32), params_all)
        grad_in, grad_params = pullback(sequence_grad.astype(jnp.float32))
        totals = tuple((running + adding for running, adding in zip(totals, grad_params)))
        return (totals, (result.astype(jnp.bfloat16), grad_in))
    totals, (output, in_grad) = lax.scan(one_sequence, starting, (inputs, out_grad))
    return (output, in_grad, totals[0], totals[1], totals[2], totals[3], totals[4], totals[5], totals[6], totals[7])
```

```python
import jax
import jax.numpy as jnp
from jax import lax
from jax.sharding import PartitionSpec as P

EPSILON = 1e-05


def shifted(block, axis, distance):
    devices = range(lax.axis_size(axis))
    route = [(i - distance, i) for i in devices if i - distance in devices]
    return lax.ppermute(block, axis, route)


DIMS = {16: (4, 2, 2), 64: (4, 4, 4)}


def seq_dims():
    n = lax.axis_size("seq")
    return DIMS.get(n, (n,))


def pair_sum(part):
    return part + lax.ppermute(part, "tensor", [(0, 1), (1, 0)])


def pair_sum_low(part):
    low = lax.optimization_barrier(part.astype(jnp.bfloat16))
    other = lax.ppermute(low, "tensor", [(0, 1), (1, 0)])
    return low.astype(jnp.float32) + other.astype(jnp.float32)


def hop(block, dims, dim, step, spots):
    n = lax.axis_size("seq")
    stride = 1
    for size in dims[dim + 1 :]:
        stride *= size
    route = [(i, i + step * stride) for i in range(n) if (i // stride) % dims[dim] in spots]
    return lax.ppermute(block, "seq", route)


def scatter_sum(whole, order, wire=jnp.bfloat16):
    dims = seq_dims()
    rest = whole.shape[1:]
    rows = whole.shape[0] // lax.axis_size("seq")
    index = lax.axis_index("seq")
    spot = []
    for size in reversed(dims):
        spot.insert(0, index % size)
        index = index // size
    parts = [(whole.reshape(dims + (rows,) + rest), list(range(len(dims))))]

    def pick(part, dim, at):
        array, left = part
        axis = left.index(dim)
        return lax.dynamic_index_in_dim(array, at, axis, keepdims=False)

    def total(parts, dim, at):
        return sum(pick(part, dim, at).astype(jnp.float32) for part in parts)

    for dim in order:
        size = dims[dim]
        here = spot[dim]
        left = [d for d in parts[0][1] if d != dim]
        if size == 2:
            sent = total(parts, dim, 1 - here).astype(wire)
            n = lax.axis_size("seq")
            stride = 1
            for other in dims[dim + 1 :]:
                stride *= other
            got = [lax.ppermute(sent, "seq", [(i, i + stride * (1 - 2 * ((i // stride) % 2))) for i in range(n)])]
        else:
            got = []
            for step in (1, -1):
                carried = None
                for distance in range(size - 1, 0, -1):
                    at = jnp.clip(here + step * distance, 0, size - 1)
                    sent = total(parts, dim, at)
                    if carried is not None:
                        sent = sent + carried.astype(jnp.float32)
                    spots = [c for c in range(size) if 0 <= c + step * distance < size]
                    carried = hop(sent.astype(wire), dims, dim, step, spots)
                got.append(carried)
        parts = [(pick(part, dim, here), left) for part in parts] + [(block, left) for block in got]
    return sum(part.astype(jnp.float32) for part, _ in parts)


def inverse_rms(stream):
    return lax.rsqrt(jnp.mean(stream * stream, axis=-1, keepdims=True) + EPSILON)


def norm_back(grad_normed, stream, inv_scale, gain_vec):
    weighted = grad_normed * gain_vec
    gain_grad = jnp.sum(grad_normed * stream * inv_scale, axis=(0, 1))
    cubed = inv_scale * inv_scale * inv_scale
    grad_before = inv_scale * weighted - stream * cubed * jnp.mean(
        weighted * stream, axis=-1, keepdims=True
    )
    return (gain_grad, grad_before)


def forward_block(stream, weights):
    gain_mix, weight_in, weight_conv, weight_out, gain_ffn, weight_gate, weight_up, weight_down = (
        weights
    )
    seq_count, rows_in, model_width = stream.shape
    channels = weight_in.shape[-1]
    hidden = weight_gate.shape[-1]
    scale_mix = inverse_rms(stream)
    normed_mix = (stream * scale_mix * gain_mix.astype(jnp.float32)).astype(jnp.bfloat16)
    projected = jnp.dot(
        normed_mix.reshape(-1, model_width),
        weight_in.reshape(model_width, 3 * channels),
        preferred_element_type=jnp.float32,
    )
    projected = projected.reshape(seq_count, rows_in, 3, channels)
    gated_in = projected[:, :, 0] * projected[:, :, 2]
    carried = shifted(gated_in[:, -2:], "seq", 1)
    extended = jnp.concatenate([carried, gated_in], axis=1)
    out_rows = extended.shape[1] - 2
    kernel = weight_conv.astype(jnp.float32)
    convolved = (
        kernel[0] * extended[:, :out_rows]
        + kernel[1] * extended[:, 1 : out_rows + 1]
        + kernel[2] * extended[:, 2:]
    )
    mixed_out = (projected[:, -out_rows:, 1] * convolved).astype(jnp.bfloat16)
    partial_out = jnp.dot(
        mixed_out.reshape(-1, channels), weight_out, preferred_element_type=jnp.float32
    )
    middle = stream + pair_sum(partial_out).reshape(seq_count, out_rows, model_width)
    scale_ffn = inverse_rms(middle)
    normed_ffn = (middle * scale_ffn * gain_ffn.astype(jnp.float32)).astype(jnp.bfloat16)
    flat_ffn = normed_ffn.reshape(-1, model_width)
    gate_pre = jnp.dot(flat_ffn, weight_gate, preferred_element_type=jnp.float32)
    up_pre = jnp.dot(flat_ffn, weight_up, preferred_element_type=jnp.float32)
    activated = (jax.nn.silu(gate_pre) * up_pre).astype(jnp.bfloat16)
    partial_ffn = jnp.dot(activated, weight_down, preferred_element_type=jnp.float32)
    result = middle + pair_sum_low(partial_ffn).reshape(seq_count, out_rows, model_width)
    stored = (
        stream,
        scale_mix,
        normed_mix,
        projected,
        extended,
        convolved,
        mixed_out,
        middle,
        scale_ffn,
        normed_ffn,
        gate_pre.reshape(seq_count, out_rows, hidden),
        up_pre.reshape(seq_count, out_rows, hidden),
        activated.reshape(seq_count, out_rows, hidden),
    )
    return (result, stored)


def backward_ffn(grad_stream, stored, weights):
    gain_mix, weight_in, weight_conv, weight_out, gain_ffn, weight_gate, weight_up, weight_down = (
        weights
    )
    (
        block_in,
        scale_mix,
        normed_mix,
        projected,
        extended,
        convolved,
        mixed_out,
        middle,
        scale_ffn,
        normed_ffn,
        gate_pre,
        up_pre,
        activated,
    ) = stored
    seq_count, own_len, model_width = grad_stream.shape
    hidden = weight_gate.shape[-1]
    rounded = grad_stream.astype(jnp.bfloat16).reshape(-1, model_width)
    grad_hidden = jnp.einsum("nd,fd->nf", rounded, weight_down, preferred_element_type=jnp.float32)
    down_grad = jnp.einsum(
        "nf,nd->fd", activated.reshape(-1, hidden), rounded, preferred_element_type=jnp.float32
    )
    gate_flat = gate_pre.reshape(-1, hidden)
    up_flat = up_pre.reshape(-1, hidden)
    sigmoid_gate = jax.nn.sigmoid(gate_flat)
    grad_gate = (
        grad_hidden * up_flat * sigmoid_gate * (1.0 + gate_flat * (1.0 - sigmoid_gate))
    ).astype(jnp.bfloat16)
    grad_up = (grad_hidden * gate_flat * sigmoid_gate).astype(jnp.bfloat16)
    flat_ffn = normed_ffn.reshape(-1, model_width)
    gate_grad = jnp.einsum("nd,nf->df", flat_ffn, grad_gate, preferred_element_type=jnp.float32)
    up_grad = jnp.einsum("nd,nf->df", flat_ffn, grad_up, preferred_element_type=jnp.float32)
    partial_ffn = jnp.einsum(
        "nf,df->nd", grad_gate, weight_gate, preferred_element_type=jnp.float32
    )
    partial_ffn = partial_ffn + jnp.einsum(
        "nf,df->nd", grad_up, weight_up, preferred_element_type=jnp.float32
    )
    grad_normed = pair_sum(partial_ffn).reshape(seq_count, own_len, model_width)
    ffn_gain_grad, grad_middle = norm_back(
        grad_normed, middle, scale_ffn, gain_ffn.astype(jnp.float32)
    )
    grad_middle = grad_stream + grad_middle
    return (grad_middle, (ffn_gain_grad, gate_grad, up_grad, down_grad))


def backward_mixer(grad_middle, stored, weights):
    gain_mix, weight_in, weight_conv, weight_out, gain_ffn, weight_gate, weight_up, weight_down = (
        weights
    )
    (
        block_in,
        scale_mix,
        normed_mix,
        projected,
        extended,
        convolved,
        mixed_out,
        middle,
        scale_ffn,
        normed_ffn,
        gate_pre,
        up_pre,
        activated,
    ) = stored
    seq_count, own_len, model_width = grad_middle.shape
    channels = weight_out.shape[0]
    rounded_mid = grad_middle.astype(jnp.bfloat16).reshape(-1, model_width)
    grad_mixed = jnp.einsum(
        "nd,cd->nc", rounded_mid, weight_out, preferred_element_type=jnp.float32
    )
    grad_mixed = grad_mixed.reshape(seq_count, own_len, channels)
    out_grad_w = jnp.einsum(
        "nc,nd->cd",
        mixed_out.reshape(-1, channels),
        rounded_mid,
        preferred_element_type=jnp.float32,
    )
    grad_conv = grad_mixed * projected[:, :, 1]
    grad_second = grad_mixed * convolved
    following = shifted(grad_conv[:, :2], "seq", -1)
    ext_grad = jnp.concatenate([grad_conv, following], axis=1)
    kernel = weight_conv.astype(jnp.float32)
    grad_gated = (
        kernel[0] * ext_grad[:, 2:] + kernel[1] * ext_grad[:, 1:-1] + kernel[2] * ext_grad[:, :-2]
    )
    conv_grad = jnp.stack(
        [
            jnp.sum(grad_conv * extended[:, offset : offset + own_len], axis=(0, 1))
            for offset in range(3)
        ]
    )
    grad_proj = jnp.stack(
        [grad_gated * projected[:, :, 2], grad_second, grad_gated * projected[:, :, 0]], axis=2
    )
    grad_proj = grad_proj.astype(jnp.bfloat16).reshape(-1, 3 * channels)
    in_grad_w = jnp.einsum(
        "nd,nk->dk",
        normed_mix.reshape(-1, model_width),
        grad_proj,
        preferred_element_type=jnp.float32,
    )
    in_grad_w = in_grad_w.reshape(model_width, 3, channels)
    partial_mix = jnp.einsum(
        "nk,dk->nd",
        grad_proj,
        weight_in.reshape(model_width, 3 * channels),
        preferred_element_type=jnp.float32,
    )
    grad_normed_mix = (
        pair_sum_low(partial_mix)
        .reshape(seq_count, own_len, model_width)
    )
    mix_gain_grad, grad_input = norm_back(
        grad_normed_mix, block_in, scale_mix, gain_mix.astype(jnp.float32)
    )
    grad_input = grad_middle + grad_input
    return (grad_input, (mix_gain_grad, in_grad_w, conv_grad, out_grad_w))


def local(
    inputs,
    out_grad,
    mix_gain,
    in_weight,
    conv_weight,
    out_weight,
    ffn_gain,
    gate_weight,
    up_weight,
    down_weight,
):
    layer_count = mix_gain.shape[0]

    def weights_of(number):
        return (
            mix_gain[number],
            in_weight[number],
            conv_weight[number],
            out_weight[number],
            ffn_gain[number],
            gate_weight[number],
            up_weight[number],
            down_weight[number],
        )

    stream = inputs.astype(jnp.float32)
    number = 0
    stream, stored = forward_block(stream, weights_of(number))
    stored_all = [stored]
    output = stream.astype(jnp.bfloat16)
    grad_stream = out_grad.astype(jnp.float32)
    ffn_parts = [None] * layer_count
    mixer_parts = [None] * layer_count
    for number in reversed(range(layer_count)):
        grad_middle, ffn_terms = backward_ffn(grad_stream, stored_all[number], weights_of(number))
        ffn_parts[number] = ffn_terms
        grad_stream, mixer_terms = backward_mixer(
            grad_middle, stored_all[number], weights_of(number)
        )
        mixer_parts[number] = mixer_terms
    joined = tuple(mixer_parts[0]) + tuple(ffn_parts[0])
    mix_gain_g, in_g, conv_g, out_g, ffn_gain_g, gate_g, up_g, down_g = joined
    n = lax.axis_size("seq")
    down_s = scatter_sum(down_g.astype(jnp.bfloat16), (0, 1, 2))
    gate_s = scatter_sum(gate_g.astype(jnp.bfloat16), (2, 1, 0))
    up_s = scatter_sum(up_g.astype(jnp.bfloat16), (1, 2, 0))
    out_s = scatter_sum(out_g.astype(jnp.bfloat16), (1, 2, 0))
    in_s = scatter_sum(in_g.astype(jnp.bfloat16), (2, 1, 0))
    taps, channels = conv_g.shape
    small = jnp.concatenate(
        [
            mix_gain_g.reshape(n, -1),
            ffn_gain_g.reshape(n, -1),
            conv_g.reshape(taps, n, -1).swapaxes(0, 1).reshape(n, -1),
        ],
        axis=1,
    )
    small = scatter_sum(small, (2, 1, 0), jnp.float32).reshape(-1)
    gain_len = mix_gain_g.shape[0] // n
    return (
        output,
        grad_stream,
        small[:gain_len][None],
        in_s[None],
        small[2 * gain_len :].reshape(1, taps, channels // n),
        out_s[None],
        small[gain_len : 2 * gain_len][None],
        gate_s[None],
        up_s[None],
        down_s[None],
    )


def solution(mesh):
    in_specs = (
        P(None, "seq", None),
        P(None, "seq", None),
        P(),
        P(None, None, None, "tensor"),
        P(None, None, "tensor"),
        P(None, "tensor", None),
        P(),
        P(None, None, "tensor"),
        P(None, None, "tensor"),
        P(None, "tensor", None),
    )
    out_specs = (
        P(None, "seq", None),
        P(None, "seq", None),
        P(None, "seq"),
        P(None, "seq", None, "tensor"),
        P(None, None, ("tensor", "seq")),
        P(None, ("tensor", "seq"), None),
        P(None, "seq"),
        P(None, "seq", "tensor"),
        P(None, "seq", "tensor"),
        P(None, ("tensor", "seq"), None),
    )
    return jax.shard_map(local, mesh=mesh, in_specs=in_specs, out_specs=out_specs, check_vma=False)
```

```python
import functools

import jax
import jax.numpy as jnp
from jax import lax
from jax.experimental import pallas as pl
from jax.experimental.pallas import tpu as pltpu
from jax.sharding import PartitionSpec as P

EPSILON = 1e-05


def shifted(block, axis, distance):
    devices = range(lax.axis_size(axis))
    route = [(i - distance, i) for i in devices if i - distance in devices]
    return lax.ppermute(block, axis, route)


DIMS = {16: (4, 2, 2), 64: (4, 4, 4)}


def seq_dims():
    n = lax.axis_size("seq")
    return DIMS.get(n, (n,))


def pair_sum(part):
    return part + lax.ppermute(part, "tensor", [(0, 1), (1, 0)])


def pair_sum_low(part):
    low = lax.optimization_barrier(part.astype(jnp.bfloat16))
    other = lax.ppermute(low, "tensor", [(0, 1), (1, 0)])
    return low.astype(jnp.float32) + other.astype(jnp.float32)


def hop(block, dims, dim, step, spots):
    n = lax.axis_size("seq")
    stride = 1
    for size in dims[dim + 1 :]:
        stride *= size
    route = [(i, i + step * stride) for i in range(n) if (i // stride) % dims[dim] in spots]
    return lax.ppermute(block, "seq", route)


def scatter_sum(whole, order, wire=jnp.bfloat16):
    dims = seq_dims()
    rest = whole.shape[1:]
    rows = whole.shape[0] // lax.axis_size("seq")
    index = lax.axis_index("seq")
    spot = []
    for size in reversed(dims):
        spot.insert(0, index % size)
        index = index // size
    parts = [(whole.reshape(dims + (rows,) + rest), list(range(len(dims))))]

    def pick(part, dim, at):
        array, left = part
        axis = left.index(dim)
        return lax.dynamic_index_in_dim(array, at, axis, keepdims=False)

    def total(parts, dim, at):
        return sum(pick(part, dim, at).astype(jnp.float32) for part in parts)

    for dim in order:
        size = dims[dim]
        here = spot[dim]
        left = [d for d in parts[0][1] if d != dim]
        if size == 2:
            sent = total(parts, dim, 1 - here).astype(wire)
            n = lax.axis_size("seq")
            stride = 1
            for other in dims[dim + 1 :]:
                stride *= other
            got = [lax.ppermute(sent, "seq", [(i, i + stride * (1 - 2 * ((i // stride) % 2))) for i in range(n)])]
        else:
            got = []
            for step in (1, -1):
                carried = None
                for distance in range(size - 1, 0, -1):
                    at = jnp.clip(here + step * distance, 0, size - 1)
                    sent = total(parts, dim, at)
                    if carried is not None:
                        sent = sent + carried.astype(jnp.float32)
                    spots = [c for c in range(size) if 0 <= c + step * distance < size]
                    carried = hop(sent.astype(wire), dims, dim, step, spots)
                got.append(carried)
        parts = [(pick(part, dim, here), left) for part in parts] + [(block, left) for block in got]
    return sum(part.astype(jnp.float32) for part, _ in parts)


MESH = pl.DeviceIdType.MESH
VMEM_BYTES = 67043328


class Unit:
    def __init__(self, member, start, width, x_first):
        self.member, self.start, self.width, self.x_first = member, start, width, x_first


def device_of(z, y, x):
    return {"seq": z * 4 + y * 2 + x}


def scatter_kernel(units, members, *refs):
    part_refs, out_refs = refs[:members], refs[members : 2 * members]
    refs = refs[2 * members :]
    count = len(units)
    first, second, third = refs[:count], refs[count : 2 * count], refs[2 * count : 3 * count]
    send1, recv1, send2, recv2, send3, recv3 = refs[3 * count :]
    me = lax.axis_index("seq")
    z, y, x = me // 4, (me // 2) % 2, me % 2

    def own(u, at_z, at_y, at_x):
        unit = units[u]
        return part_refs[unit.member].at[at_z, at_y, at_x, :, pl.ds(unit.start, unit.width)]

    def stage1(u):
        unit = units[u]
        cols = pl.ds(unit.start, unit.width)
        if unit.x_first:
            source, target = part_refs[unit.member].at[:, :, 1 - x, :, cols], device_of(z, y, 1 - x)
        else:
            source, target = part_refs[unit.member].at[:, 1 - y, :, :, cols], device_of(z, 1 - y, x)
        return pltpu.make_async_remote_copy(
            source, first[u], send1.at[u], recv1.at[u], device_id=target, device_id_type=MESH
        )

    def stage2(u):
        unit = units[u]
        if unit.x_first:
            source, target = first[u].at[:, 1 - y], device_of(z, 1 - y, x)
        else:
            source, target = first[u].at[:, 1 - x], device_of(z, y, 1 - x)
        return pltpu.make_async_remote_copy(
            source, second[u], send2.at[u], recv2.at[u], device_id=target, device_id_type=MESH
        )

    def stage3(u, d):
        other = (z + d) % 4
        return pltpu.make_async_remote_copy(
            second[u].at[other], third[u].at[d - 1], send3.at[u, d - 1], recv3.at[u, d - 1],
            device_id=device_of(other, y, x), device_id_type=MESH,
        )

    def run2(u):
        unit = units[u]
        stage1(u).wait_recv()

        @pl.loop(0, 4)
        def _(at):
            if unit.x_first:
                mine, spot = own(u, at, 1 - y, x), first[u].at[at, 1 - y]
            else:
                mine, spot = own(u, at, y, 1 - x), first[u].at[at, 1 - x]
            spot[...] = (mine[...].astype(jnp.float32) + spot[...].astype(jnp.float32)).astype(spot.dtype)

        stage2(u).start()

    def kept(u, at):
        unit = units[u]
        near = first[u].at[at, y if unit.x_first else x]
        return (
            own(u, at, y, x)[...].astype(jnp.float32)
            + near[...].astype(jnp.float32)
            + second[u].at[at][...].astype(jnp.float32)
        )

    def run3(u):
        stage2(u).wait_recv()

        @pl.loop(1, 4)
        def _(d):
            other = (z + d) % 4
            second[u].at[other][...] = kept(u, other).astype(second[u].dtype)

        for d in range(1, 4):
            stage3(u, d).start()

    def run4(u):
        unit = units[u]
        for d in range(1, 4):
            stage3(u, d).wait_recv()
        total = kept(u, z)
        for d in range(1, 4):
            total = total + third[u].at[d - 1][...].astype(jnp.float32)
        out_refs[unit.member].at[:, pl.ds(unit.start, unit.width)][...] = total

    barrier = pltpu.get_barrier_semaphore()
    for target in (device_of(z, y, 1 - x), device_of(z, 1 - y, x), *(device_of((z + d) % 4, y, x) for d in range(1, 4))):
        pl.semaphore_signal(barrier, inc=1, device_id=target, device_id_type=MESH)
    pl.semaphore_wait(barrier, 5)

    AHEAD, LAG = 4, 2
    for u in range(min(AHEAD, count)):
        stage1(u).start()
    for step in range(count + 2 * LAG):
        if step < count:
            run2(step)
            if step + AHEAD < count:
                stage1(step + AHEAD).start()
        if 0 <= step - LAG < count:
            run3(step - LAG)
        if 0 <= step - 2 * LAG < count:
            run4(step - 2 * LAG)
    for u in range(count):
        stage1(u).wait_send()
        stage2(u).wait_send()
        for d in range(1, 4):
            stage3(u, d).wait_send()


def scatter_all(parts, units):
    count = len(units)

    def buffer(unit, lead):
        part = parts[unit.member]
        return pltpu.VMEM((*lead, part.shape[3], unit.width), part.dtype)

    return pl.pallas_call(
        functools.partial(scatter_kernel, units, len(parts)),
        out_shape=[jax.ShapeDtypeStruct(part.shape[3:], jnp.float32) for part in parts],
        in_specs=[pl.BlockSpec(memory_space=pltpu.VMEM)] * len(parts),
        out_specs=[pl.BlockSpec(memory_space=pltpu.VMEM)] * len(parts),
        scratch_shapes=[buffer(unit, (4, 2)) for unit in units]
        + [buffer(unit, (4,)) for unit in units]
        + [buffer(unit, (3,)) for unit in units]
        + [pltpu.SemaphoreType.DMA((count,))] * 4
        + [pltpu.SemaphoreType.DMA((count, 3))] * 2,
        compiler_params=pltpu.CompilerParams(
            collective_id=0, has_side_effects=True, vmem_limit_bytes=VMEM_BYTES
        ),
    )(*parts)


def inverse_rms(stream):
    return lax.rsqrt(jnp.mean(stream * stream, axis=-1, keepdims=True) + EPSILON)


def norm_back(grad_normed, stream, inv_scale, gain_vec):
    weighted = grad_normed * gain_vec
    gain_grad = jnp.sum(grad_normed * stream * inv_scale, axis=(0, 1))
    cubed = inv_scale * inv_scale * inv_scale
    grad_before = inv_scale * weighted - stream * cubed * jnp.mean(
        weighted * stream, axis=-1, keepdims=True
    )
    return (gain_grad, grad_before)


def forward_block(stream, weights):
    gain_mix, weight_in, weight_conv, weight_out, gain_ffn, weight_gate, weight_up, weight_down = (
        weights
    )
    seq_count, rows_in, model_width = stream.shape
    channels = weight_in.shape[-1]
    hidden = weight_gate.shape[-1]
    scale_mix = inverse_rms(stream)
    normed_mix = (stream * scale_mix * gain_mix.astype(jnp.float32)).astype(jnp.bfloat16)
    projected = jnp.dot(
        normed_mix.reshape(-1, model_width),
        weight_in.reshape(model_width, 3 * channels),
        preferred_element_type=jnp.float32,
    )
    projected = projected.reshape(seq_count, rows_in, 3, channels)
    gated_in = projected[:, :, 0] * projected[:, :, 2]
    carried = shifted(gated_in[:, -2:], "seq", 1)
    extended = jnp.concatenate([carried, gated_in], axis=1)
    out_rows = extended.shape[1] - 2
    kernel = weight_conv.astype(jnp.float32)
    convolved = (
        kernel[0] * extended[:, :out_rows]
        + kernel[1] * extended[:, 1 : out_rows + 1]
        + kernel[2] * extended[:, 2:]
    )
    mixed_out = (projected[:, -out_rows:, 1] * convolved).astype(jnp.bfloat16)
    partial_out = jnp.dot(
        mixed_out.reshape(-1, channels), weight_out, preferred_element_type=jnp.float32
    )
    middle = stream + pair_sum(partial_out).reshape(seq_count, out_rows, model_width)
    scale_ffn = inverse_rms(middle)
    normed_ffn = (middle * scale_ffn * gain_ffn.astype(jnp.float32)).astype(jnp.bfloat16)
    flat_ffn = normed_ffn.reshape(-1, model_width)
    gate_pre = jnp.dot(flat_ffn, weight_gate, preferred_element_type=jnp.float32)
    up_pre = jnp.dot(flat_ffn, weight_up, preferred_element_type=jnp.float32)
    activated = (jax.nn.silu(gate_pre) * up_pre).astype(jnp.bfloat16)
    partial_ffn = jnp.dot(activated, weight_down, preferred_element_type=jnp.float32)
    result = middle + pair_sum_low(partial_ffn).reshape(seq_count, out_rows, model_width)
    stored = (
        stream,
        scale_mix,
        normed_mix,
        projected,
        extended,
        convolved,
        mixed_out,
        middle,
        scale_ffn,
        normed_ffn,
        gate_pre.reshape(seq_count, out_rows, hidden),
        up_pre.reshape(seq_count, out_rows, hidden),
        activated.reshape(seq_count, out_rows, hidden),
    )
    return (result, stored)


def backward_ffn(grad_stream, stored, weights):
    gain_mix, weight_in, weight_conv, weight_out, gain_ffn, weight_gate, weight_up, weight_down = (
        weights
    )
    (
        block_in,
        scale_mix,
        normed_mix,
        projected,
        extended,
        convolved,
        mixed_out,
        middle,
        scale_ffn,
        normed_ffn,
        gate_pre,
        up_pre,
        activated,
    ) = stored
    seq_count, own_len, model_width = grad_stream.shape
    hidden = weight_gate.shape[-1]
    rounded = grad_stream.astype(jnp.bfloat16).reshape(-1, model_width)
    grad_hidden = jnp.einsum("nd,fd->nf", rounded, weight_down, preferred_element_type=jnp.float32)
    down_grad = jnp.einsum(
        "nf,nd->fd", activated.reshape(-1, hidden), rounded, preferred_element_type=jnp.float32
    )
    gate_flat = gate_pre.reshape(-1, hidden)
    up_flat = up_pre.reshape(-1, hidden)
    sigmoid_gate = jax.nn.sigmoid(gate_flat)
    grad_gate = (
        grad_hidden * up_flat * sigmoid_gate * (1.0 + gate_flat * (1.0 - sigmoid_gate))
    ).astype(jnp.bfloat16)
    grad_up = (grad_hidden * gate_flat * sigmoid_gate).astype(jnp.bfloat16)
    flat_ffn = normed_ffn.reshape(-1, model_width)
    gate_grad = jnp.einsum("nd,nf->df", flat_ffn, grad_gate, preferred_element_type=jnp.float32)
    up_grad = jnp.einsum("nd,nf->df", flat_ffn, grad_up, preferred_element_type=jnp.float32)
    partial_ffn = jnp.einsum(
        "nf,df->nd", grad_gate, weight_gate, preferred_element_type=jnp.float32
    )
    partial_ffn = partial_ffn + jnp.einsum(
        "nf,df->nd", grad_up, weight_up, preferred_element_type=jnp.float32
    )
    grad_normed = pair_sum(partial_ffn).reshape(seq_count, own_len, model_width)
    ffn_gain_grad, grad_middle = norm_back(
        grad_normed, middle, scale_ffn, gain_ffn.astype(jnp.float32)
    )
    grad_middle = grad_stream + grad_middle
    return (grad_middle, (ffn_gain_grad, gate_grad, up_grad, down_grad))


def backward_mixer(grad_middle, stored, weights):
    gain_mix, weight_in, weight_conv, weight_out, gain_ffn, weight_gate, weight_up, weight_down = (
        weights
    )
    (
        block_in,
        scale_mix,
        normed_mix,
        projected,
        extended,
        convolved,
        mixed_out,
        middle,
        scale_ffn,
        normed_ffn,
        gate_pre,
        up_pre,
        activated,
    ) = stored
    seq_count, own_len, model_width = grad_middle.shape
    channels = weight_out.shape[0]
    rounded_mid = grad_middle.astype(jnp.bfloat16).reshape(-1, model_width)
    grad_mixed = jnp.einsum(
        "nd,cd->nc", rounded_mid, weight_out, preferred_element_type=jnp.float32
    )
    grad_mixed = grad_mixed.reshape(seq_count, own_len, channels)
    out_grad_w = jnp.einsum(
        "nc,nd->cd",
        mixed_out.reshape(-1, channels),
        rounded_mid,
        preferred_element_type=jnp.float32,
    )
    grad_conv = grad_mixed * projected[:, :, 1]
    grad_second = grad_mixed * convolved
    following = shifted(grad_conv[:, :2], "seq", -1)
    ext_grad = jnp.concatenate([grad_conv, following], axis=1)
    kernel = weight_conv.astype(jnp.float32)
    grad_gated = (
        kernel[0] * ext_grad[:, 2:] + kernel[1] * ext_grad[:, 1:-1] + kernel[2] * ext_grad[:, :-2]
    )
    conv_grad = jnp.stack(
        [
            jnp.sum(grad_conv * extended[:, offset : offset + own_len], axis=(0, 1))
            for offset in range(3)
        ]
    )
    grad_proj = jnp.stack(
        [grad_gated * projected[:, :, 2], grad_second, grad_gated * projected[:, :, 0]], axis=2
    )
    grad_proj = grad_proj.astype(jnp.bfloat16).reshape(-1, 3 * channels)
    in_grad_w = jnp.einsum(
        "nd,nk->dk",
        normed_mix.reshape(-1, model_width),
        grad_proj,
        preferred_element_type=jnp.float32,
    )
    in_grad_w = in_grad_w.reshape(model_width, 3, channels)
    partial_mix = jnp.einsum(
        "nk,dk->nd",
        grad_proj,
        weight_in.reshape(model_width, 3 * channels),
        preferred_element_type=jnp.float32,
    )
    grad_normed_mix = (
        pair_sum_low(partial_mix)
        .reshape(seq_count, own_len, model_width)
    )
    mix_gain_grad, grad_input = norm_back(
        grad_normed_mix, block_in, scale_mix, gain_mix.astype(jnp.float32)
    )
    grad_input = grad_middle + grad_input
    return (grad_input, (mix_gain_grad, in_grad_w, conv_grad, out_grad_w))


def local(
    inputs,
    out_grad,
    mix_gain,
    in_weight,
    conv_weight,
    out_weight,
    ffn_gain,
    gate_weight,
    up_weight,
    down_weight,
):
    layer_count = mix_gain.shape[0]

    def weights_of(number):
        return (
            mix_gain[number],
            in_weight[number],
            conv_weight[number],
            out_weight[number],
            ffn_gain[number],
            gate_weight[number],
            up_weight[number],
            down_weight[number],
        )

    stream = inputs.astype(jnp.float32)
    number = 0
    stream, stored = forward_block(stream, weights_of(number))
    stored_all = [stored]
    output = stream.astype(jnp.bfloat16)
    grad_stream = out_grad.astype(jnp.float32)
    ffn_parts = [None] * layer_count
    mixer_parts = [None] * layer_count
    for number in reversed(range(layer_count)):
        grad_middle, ffn_terms = backward_ffn(grad_stream, stored_all[number], weights_of(number))
        ffn_parts[number] = ffn_terms
        grad_stream, mixer_terms = backward_mixer(
            grad_middle, stored_all[number], weights_of(number)
        )
        mixer_parts[number] = mixer_terms
    joined = tuple(mixer_parts[0]) + tuple(ffn_parts[0])
    mix_gain_g, in_g, conv_g, out_g, ffn_gain_g, gate_g, up_g, down_g = joined
    n = lax.axis_size("seq")
    taps, channels = conv_g.shape
    small = jnp.concatenate(
        [
            mix_gain_g.reshape(n, -1),
            ffn_gain_g.reshape(n, -1),
            conv_g.reshape(taps, n, -1).swapaxes(0, 1).reshape(n, -1),
        ],
        axis=1,
    )
    if n == 16:
        low = [gate_g, up_g, down_g, in_g.reshape(in_g.shape[0], -1), out_g]
        parts = [g.astype(jnp.bfloat16).reshape(4, 2, 2, g.shape[0] // n, -1) for g in low]
        length = small.shape[1]
        padded = jnp.pad(small, ((0, 0), (0, 1024 - length)))
        parts.append(padded.reshape(4, 2, 2, 8, 128))
        units = [Unit(5, 0, 128, True)]
        for start in range(0, 2304, 768):
            units += [Unit(0, start, 768, True), Unit(1, start, 768, False)]
        units += [Unit(2, 0, 512, True), Unit(2, 512, 512, False)]
        units += [Unit(3, 0, 512, True), Unit(3, 512, 512, False), Unit(3, 1024, 256, True), Unit(3, 1280, 256, False)]
        units += [Unit(4, 0, 512, True), Unit(4, 512, 512, False)]
        gate_s, up_s, down_s, in_s, out_s, small = scatter_all(parts, units)
        in_s = in_s.reshape(-1, 3, in_g.shape[2])
        small = small.reshape(-1)[:length]
    else:
        down_s = scatter_sum(down_g.astype(jnp.bfloat16), (0, 1, 2))
        gate_s = scatter_sum(gate_g.astype(jnp.bfloat16), (2, 1, 0))
        up_s = scatter_sum(up_g.astype(jnp.bfloat16), (1, 2, 0))
        out_s = scatter_sum(out_g.astype(jnp.bfloat16), (1, 2, 0))
        in_s = scatter_sum(in_g.astype(jnp.bfloat16), (2, 1, 0))
        small = scatter_sum(small, (2, 1, 0), jnp.float32).reshape(-1)
    gain_len = mix_gain_g.shape[0] // n
    return (
        output,
        grad_stream,
        small[:gain_len][None],
        in_s[None],
        small[2 * gain_len :].reshape(1, taps, channels // n),
        out_s[None],
        small[gain_len : 2 * gain_len][None],
        gate_s[None],
        up_s[None],
        down_s[None],
    )


def solution(mesh):
    in_specs = (
        P(None, "seq", None),
        P(None, "seq", None),
        P(),
        P(None, None, None, "tensor"),
        P(None, None, "tensor"),
        P(None, "tensor", None),
        P(),
        P(None, None, "tensor"),
        P(None, None, "tensor"),
        P(None, "tensor", None),
    )
    out_specs = (
        P(None, "seq", None),
        P(None, "seq", None),
        P(None, "seq"),
        P(None, "seq", None, "tensor"),
        P(None, None, ("tensor", "seq")),
        P(None, ("tensor", "seq"), None),
        P(None, "seq"),
        P(None, "seq", "tensor"),
        P(None, "seq", "tensor"),
        P(None, ("tensor", "seq"), None),
    )
    return jax.shard_map(local, mesh=mesh, in_specs=in_specs, out_specs=out_specs, check_vma=False)
```

```python
import jax
import jax.numpy as jnp
from jax import lax
from jax.experimental import pallas as pl
from jax.experimental.pallas import tpu as pltpu
from jax.sharding import PartitionSpec as P

EPSILON = 1e-05


def shifted(block, axis, distance):
    devices = range(lax.axis_size(axis))
    route = [(i - distance, i) for i in devices if i - distance in devices]
    return lax.ppermute(block, axis, route)


DIMS = {16: (4, 2, 2), 64: (4, 4, 4)}


def seq_dims():
    n = lax.axis_size("seq")
    return DIMS.get(n, (n,))


def pair_sum(part):
    return part + lax.ppermute(part, "tensor", [(0, 1), (1, 0)])


def pair_sum_low(part):
    low = lax.optimization_barrier(part.astype(jnp.bfloat16))
    other = lax.ppermute(low, "tensor", [(0, 1), (1, 0)])
    return low.astype(jnp.float32) + other.astype(jnp.float32)


def hop(block, dims, dim, step, spots):
    n = lax.axis_size("seq")
    stride = 1
    for size in dims[dim + 1 :]:
        stride *= size
    route = [(i, i + step * stride) for i in range(n) if (i // stride) % dims[dim] in spots]
    return lax.ppermute(block, "seq", route)


def scatter_sum(whole, order, wire=jnp.bfloat16):
    dims = seq_dims()
    rest = whole.shape[1:]
    rows = whole.shape[0] // lax.axis_size("seq")
    index = lax.axis_index("seq")
    spot = []
    for size in reversed(dims):
        spot.insert(0, index % size)
        index = index // size
    parts = [(whole.reshape(dims + (rows,) + rest), list(range(len(dims))))]

    def pick(part, dim, at):
        array, left = part
        axis = left.index(dim)
        return lax.dynamic_index_in_dim(array, at, axis, keepdims=False)

    def total(parts, dim, at):
        return sum(pick(part, dim, at).astype(jnp.float32) for part in parts)

    for dim in order:
        size = dims[dim]
        here = spot[dim]
        left = [d for d in parts[0][1] if d != dim]
        if size == 2:
            sent = total(parts, dim, 1 - here).astype(wire)
            n = lax.axis_size("seq")
            stride = 1
            for other in dims[dim + 1 :]:
                stride *= other
            got = [lax.ppermute(sent, "seq", [(i, i + stride * (1 - 2 * ((i // stride) % 2))) for i in range(n)])]
        else:
            got = []
            for step in (1, -1):
                carried = None
                for distance in range(size - 1, 0, -1):
                    at = jnp.clip(here + step * distance, 0, size - 1)
                    sent = total(parts, dim, at)
                    if carried is not None:
                        sent = sent + carried.astype(jnp.float32)
                    spots = [c for c in range(size) if 0 <= c + step * distance < size]
                    carried = hop(sent.astype(wire), dims, dim, step, spots)
                got.append(carried)
        parts = [(pick(part, dim, here), left) for part in parts] + [(block, left) for block in got]
    return sum(part.astype(jnp.float32) for part, _ in parts)


MESH = pl.DeviceIdType.MESH
VMEM_BYTES = 67043328
F32, BF16 = jnp.float32, jnp.bfloat16
WIDE = 256


def times(a, b):
    return jnp.dot(a, b, preferred_element_type=F32)


def times_t(a, b):
    return lax.dot_general(a, b, (((1,), (1,)), ((), ())), preferred_element_type=F32)


def device_of(z, y, x):
    return {"seq": z * 4 + y * 2 + x}


class Scatter:
    def __init__(self, base, part, first, second, third, sems):
        self.base, self.part = base, part
        self.first, self.second, self.third = first, second, third
        self.send1, self.recv1, self.send2, self.recv2, self.send3, self.recv3 = sems
        me = lax.axis_index("seq")
        self.z, self.y, self.x = me // 4, (me // 2) % 2, me % 2

    def stage1(self, u, x_first):
        z, y, x = self.z, self.y, self.x
        if x_first:
            source, target = self.part.at[u, :, :, 1 - x], device_of(z, y, 1 - x)
        else:
            source, target = self.part.at[u, :, 1 - y], device_of(z, 1 - y, x)
        k = self.base + u
        return pltpu.make_async_remote_copy(
            source, self.first.at[u], self.send1.at[k], self.recv1.at[k], device_id=target, device_id_type=MESH
        )

    def stage2(self, u, x_first):
        z, y, x = self.z, self.y, self.x
        if x_first:
            source, target = self.first.at[u, :, 1 - y], device_of(z, 1 - y, x)
        else:
            source, target = self.first.at[u, :, 1 - x], device_of(z, y, 1 - x)
        k = self.base + u
        return pltpu.make_async_remote_copy(
            source, self.second.at[u], self.send2.at[k], self.recv2.at[k], device_id=target, device_id_type=MESH
        )

    def stage3(self, u, d):
        other = (self.z + d) % 4
        k = self.base + u
        return pltpu.make_async_remote_copy(
            self.second.at[u, other], self.third.at[u, d - 1], self.send3.at[k, d - 1], self.recv3.at[k, d - 1],
            device_id=device_of(other, self.y, self.x), device_id_type=MESH,
        )

    def run1(self, u, x_first):
        self.stage1(u, x_first).start()

    def run2(self, u, x_first):
        y, x = self.y, self.x
        self.stage1(u, x_first).wait_recv()

        @pl.loop(0, 4)
        def _(at):
            if x_first:
                mine, spot = self.part.at[u, at, 1 - y, x], self.first.at[u, at, 1 - y]
            else:
                mine, spot = self.part.at[u, at, y, 1 - x], self.first.at[u, at, 1 - x]
            spot[...] = (mine[...].astype(F32) + spot[...].astype(F32)).astype(spot.dtype)

        self.stage2(u, x_first).start()

    def kept(self, u, x_first, at):
        y, x = self.y, self.x
        near = self.first.at[u, at, y if x_first else x]
        return (
            self.part[u, at, y, x].astype(F32) + near[...].astype(F32) + self.second[u, at].astype(F32)
        )

    def run3(self, u, x_first):
        self.stage2(u, x_first).wait_recv()

        @pl.loop(1, 4)
        def _(d):
            other = (self.z + d) % 4
            self.second[u, other] = self.kept(u, x_first, other).astype(self.second.dtype)

        for d in range(1, 4):
            self.stage3(u, d).start()

    def run4(self, u, x_first):
        for d in range(1, 4):
            self.stage3(u, d).wait_recv()
        total = self.kept(u, x_first, self.z)
        for d in range(1, 4):
            total = total + self.third[u, d - 1].astype(F32)
        return total

    def drain(self, u, x_first):
        self.stage1(u, x_first).wait_send()
        self.stage2(u, x_first).wait_send()
        for d in range(1, 4):
            self.stage3(u, d).wait_send()


def block_kernel(
    x_hbm, og_hbm, win_hbm, wout_hbm, wg_hbm, wu_hbm, wd_hbm, gain_mix, taps, gain_ffn,
    out_hbm, in_grad_hbm, gate_hbm, up_hbm, down_hbm, in_hbm, outw_hbm, small_hbm,
    og, acts, nt, mid, proj, gext, gcon, mixed, wout, wbuf, wdbuf, out_acc, gn_acc,
    sa, sb, ra, rb, gp, hid, sums, taps_sum,
    part_q, first_q, second_q, third_q,
    part_d, first_d, second_d, third_d,
    part_o, first_o, second_o, third_o,
    part_s, first_s, second_s, third_s,
    stage_q, stage_d, stage_o, stage_s,
    send1, recv1, send2, recv2, send3, recv3,
    load_sem, w_sem, wd_sem, ex_send, ex_recv, halo_send, halo_recv, store_sem,
):
    rows, width = og.shape
    me = lax.axis_index("seq")
    last = lax.axis_size("seq") - 1
    core = lax.axis_index("tensor")
    chunks = wd_hbm.shape[0] // WIDE
    cols = width // WIDE
    sems = (send1, recv1, send2, recv2, send3, recv3)
    quads = Scatter(0, part_q, first_q, second_q, third_q, sems)
    downs = Scatter(24, part_d, first_d, second_d, third_d, sems)
    outs = Scatter(28, part_o, first_o, second_o, third_o, sems)
    smalls = Scatter(32, part_s, first_s, second_s, third_s, sems)

    def load(index, source, target):
        return pltpu.make_async_copy(source, target, load_sem.at[index])

    def win(i, slot):
        return pltpu.make_async_copy(win_hbm.at[:, pl.ds(i * WIDE, WIDE)], wbuf.at[slot], w_sem.at[slot])

    def wgate(j, slot):
        return pltpu.make_async_copy(wg_hbm.at[:, pl.ds(pl.multiple_of(j * WIDE, WIDE), WIDE)], wbuf.at[slot], w_sem.at[slot])

    def wup(j, slot):
        return pltpu.make_async_copy(wu_hbm.at[:, pl.ds(pl.multiple_of(j * WIDE, WIDE), WIDE)], wbuf.at[slot], w_sem.at[slot])

    def wdown(j, slot):
        return pltpu.make_async_copy(wd_hbm.at[pl.ds(pl.multiple_of(j * WIDE, WIDE), WIDE)], wdbuf.at[slot], wd_sem.at[slot])

    order = (0, 4, 1, 5, 2, 3)
    load(0, x_hbm, sb).start()
    for place in range(4):
        win(order[place], place).start()
    load(1, og_hbm, og).start()
    load(2, wout_hbm, wout).start()
    wdown(0, 0).start()

    barrier = pltpu.get_barrier_semaphore()
    z, y, x = quads.z, quads.y, quads.x
    near = [device_of(z, y, 1 - x), device_of(z, 1 - y, x), *(device_of((z + d) % 4, y, x) for d in range(1, 4))]
    near += [{"tensor": 1 - core}, {"seq": (me + last) % (last + 1)}, {"seq": (me + 1) % (last + 1)}]
    for target in near:
        pl.semaphore_signal(barrier, inc=1, device_id=target, device_id_type=MESH)

    load(0, x_hbm, sb).wait()

    @pl.loop(0, rows // 16)
    def _(r):
        at = pl.ds(pl.multiple_of(r * 16, 16), 16)
        stream = sb[at, :].astype(F32)
        scale = lax.rsqrt(jnp.mean(stream * stream, axis=-1, keepdims=True) + EPSILON)
        acts[at, :] = (stream * scale * gain_mix[...].astype(F32)).astype(BF16)

    pl.semaphore_wait(barrier, len(near))

    def halo_fwd(c):
        return pltpu.make_async_remote_copy(
            gext.at[c, pl.ds(rows, 8)], gext.at[c, pl.ds(0, 8)], halo_send.at[c], halo_recv.at[c],
            device_id={"seq": me + 1}, device_id_type=MESH,
        )

    def halo_back(c):
        return pltpu.make_async_remote_copy(
            gcon.at[c, pl.ds(0, 8)], gcon.at[c, pl.ds(rows, 8)], halo_send.at[2 + c], halo_recv.at[2 + c],
            device_id={"seq": me - 1}, device_id_type=MESH,
        )

    for place, i in enumerate(order):
        slot = place % 4
        win(i, slot).wait()
        proj[i] = times(acts[...], wbuf[slot])
        if place + 4 < len(order):
            win(order[place + 4], slot).start()
        if i >= 4:
            c = i - 4

            @pl.loop(0, rows // 64)
            def _(r):
                at = pl.ds(pl.multiple_of(r * 64, 64), 64)
                to = pl.ds(pl.multiple_of(r * 64 + 8, 8), 64)
                gext[c, to, :] = proj[c, at, :] * proj[4 + c, at, :]

            @pl.when(me < last)
            def _():
                halo_fwd(c).start()

            @pl.when(me == 0)
            def _():
                gext[c, 0:8, :] = jnp.zeros((8, WIDE), F32)

    wgate(0, 0).start()
    wup(0, 2).start()

    def tap(k, c):
        return taps[k : k + 1, c * WIDE : (c + 1) * WIDE].astype(F32)

    def convolved(c, r):
        span = gext[c, pl.ds(pl.multiple_of(r * 64, 64), 72), :]
        return tap(0, c) * span[6:70] + tap(1, c) * span[7:71] + tap(2, c) * span[8:72]

    for c in range(2):

        @pl.when(me > 0)
        def _():
            halo_fwd(c).wait_recv()

        @pl.loop(0, rows // 64)
        def _(r):
            at = pl.ds(pl.multiple_of(r * 64, 64), 64)
            mixed[c, at, :] = (proj[2 + c, at, :] * convolved(c, r)).astype(BF16)

    def exchange(index, source, target, q):
        span = pl.ds(q * WIDE, WIDE)
        return pltpu.make_async_remote_copy(
            source.at[:, span], target.at[:, span], ex_send.at[index, q], ex_recv.at[index, q],
            device_id={"tensor": 1 - core}, device_id_type=MESH,
        )

    load(2, wout_hbm, wout).wait()
    for q in range(cols):
        span = slice(q * WIDE, (q + 1) * WIDE)
        half = mixed.shape[2]
        sa[:, span] = (times(mixed[0], wout[0:half, span]) + times(mixed[1], wout[half : 2 * half, span])).astype(BF16)
        exchange(0, sa, ra, q).start()
    for q in range(cols):
        exchange(0, sa, ra, q).wait_recv()

    def mean_of(value):
        return jnp.mean(value, axis=-1, keepdims=True)

    @pl.loop(0, rows // 16)
    def _(r):
        at = pl.ds(pl.multiple_of(r * 16, 16), 16)
        stream = sb[at, :].astype(F32) + (sa[at, :].astype(F32) + ra[at, :].astype(F32))
        mid[at, :] = stream
        scale = lax.rsqrt(mean_of(stream * stream) + EPSILON)
        acts[at, :] = (stream * scale * gain_ffn[...].astype(F32)).astype(BF16)

    @pl.loop(0, rows // 128)
    def _(r):
        at = pl.ds(pl.multiple_of(r * 128, 128), 128)
        nt[:, at] = acts[at, :].T

    out_acc[...] = jnp.zeros_like(out_acc)
    gn_acc[...] = jnp.zeros_like(gn_acc)
    load(1, og_hbm, og).wait()

    @pl.loop(0, chunks)
    def _(j):
        slot = j % 2
        wgate(j, slot).wait()
        wup(j, 2 + slot).wait()
        wdown(j, slot).wait()

        @pl.when(j + 1 < chunks)
        def _():
            wgate(j + 1, 1 - slot).start()
            wup(j + 1, 3 - slot).start()
            wdown(j + 1, 1 - slot).start()

        hid[0] = times(acts[...], wbuf[slot])
        hid[1] = times(acts[...], wbuf[2 + slot])
        hid[2] = times_t(og[...], wdbuf[slot])

        @pl.loop(0, rows // 32)
        def _(r):
            at = pl.ds(pl.multiple_of(r * 32, 32), 32)
            gate, up, back = hid[0, at, :], hid[1, at, :], hid[2, at, :]
            s = jax.nn.sigmoid(gate)
            silu = gate * s
            gp[0, at, :] = (silu * up).astype(BF16)
            gp[1, at, :] = (back * up * s * (1.0 + gate * (1.0 - s))).astype(BF16)
            gp[2, at, :] = (back * silu).astype(BF16)

        part_q[j] = times(nt[...], gp[1]).astype(BF16).reshape(part_q.shape[1:])
        quads.run1(j, True)
        part_q[chunks + j] = times(nt[...], gp[2]).astype(BF16).reshape(part_q.shape[1:])
        quads.run1(chunks + j, False)
        act_t = gp[0].T
        for q in range(cols):
            block = times(act_t, og[:, q * WIDE : (q + 1) * WIDE]).astype(BF16)
            for g in range(WIDE // 16):
                group = j * (WIDE // 16) + g
                shard, row = group // 9, pl.multiple_of((group % 9) * 16, 16)
                part_d[q, shard // 4, (shard // 2) % 2, shard % 2, pl.ds(row, 16), :] = block[g * 16 : (g + 1) * 16]
        for q in range(cols):
            span = slice(q * WIDE, (q + 1) * WIDE)
            gn_acc[:, span] += times_t(gp[1], wbuf[slot, span, :]) + times_t(gp[2], wbuf[2 + slot, span, :])
            out_acc[:, span] += times(gp[0], wdbuf[slot, :, span])

        @pl.when(j >= 4)
        def _():
            quads.run2(j - 4, True)
            quads.run2(chunks + j - 4, False)

    for q in range(cols):
        downs.run1(q, q % 2 == 0)

    for q in range(cols):
        span = slice(q * WIDE, (q + 1) * WIDE)
        sb[:, span] = gn_acc[:, span].astype(BF16)
        exchange(1, sb, rb, q).start()
    for q in range(cols):
        exchange(0, sa, ra, q).wait_send()
    sa[...] = out_acc[...].astype(BF16)
    for slot, i in enumerate((0, 1, 2, 3)):
        win(i, slot).start()
    sums[...] = jnp.zeros_like(sums)
    for q in range(cols):
        exchange(1, sb, rb, q).wait_recv()

    def fold(value):
        return value[0:8] + value[8:16]

    @pl.loop(0, rows // 16)
    def _(r):
        at = pl.ds(pl.multiple_of(r * 16, 16), 16)
        grad = sb[at, :].astype(F32) + rb[at, :].astype(F32)
        stream = mid[at, :]
        scale = lax.rsqrt(mean_of(stream * stream) + EPSILON)
        weighted = grad * gain_ffn[...].astype(F32)
        sums[1] += fold(grad * stream * scale)
        middle = og[at, :].astype(F32) + (
            scale * weighted - stream * (scale * scale * scale) * mean_of(weighted * stream)
        )
        gn_acc[at, :] = middle
        acts[at, :] = middle.astype(BF16)

    for q in range(cols):
        exchange(2, sa, ra, q).start()

    load(3, x_hbm, og).start()
    half = mixed.shape[2]
    for c in range(2):
        hid[c] = times_t(acts[...], wout[c * half : (c + 1) * half, :])

        @pl.loop(0, rows // 64)
        def _(r):
            at = pl.ds(pl.multiple_of(r * 64, 64), 64)
            grad = hid[c, at, :]
            gcon[c, at, :] = grad * proj[2 + c, at, :]
            gp[2 + c, at, :] = (grad * convolved(c, r)).astype(BF16)

        @pl.when(me > 0)
        def _():
            halo_back(c).start()

        @pl.when(me == last)
        def _():
            gcon[c, rows : rows + 8, :] = jnp.zeros((8, WIDE), F32)

    for c in range(2):
        mixed_t = mixed[c].T
        for q in range(cols):
            block = times(mixed_t, acts[:, q * WIDE : (q + 1) * WIDE]).astype(BF16)
            part_o[q, 2 * c : 2 * c + 2] = block.reshape(2, *part_o.shape[2:])
    for q in range(cols):
        outs.run1(q, q % 2 == 1)

    load(3, x_hbm, og).wait()

    @pl.loop(0, rows // 128)
    def _(r):
        at = pl.ds(pl.multiple_of(r * 128, 128), 128)
        stream = og[at, :].astype(F32)
        scale = lax.rsqrt(mean_of(stream * stream) + EPSILON)
        nt[:, at] = (stream * scale * gain_mix[...].astype(F32)).astype(BF16).T

    for c in range(2):

        @pl.when(me < last)
        def _():
            halo_back(c).wait_recv()

        taps_sum[c] = jnp.zeros_like(taps_sum[c])

        @pl.loop(0, rows // 64)
        def _(r):
            at = pl.ds(pl.multiple_of(r * 64, 64), 64)
            ahead = gcon[c, pl.ds(pl.multiple_of(r * 64, 64), 72), :]
            behind = gext[c, pl.ds(pl.multiple_of(r * 64, 64), 72), :]
            grad = ahead[0:64]
            gated = tap(0, c) * ahead[2:66] + tap(1, c) * ahead[1:65] + tap(2, c) * grad
            for k in range(3):
                product = (grad * behind[6 + k : 70 + k]).reshape(8, 8, WIDE)
                taps_sum[c, k] += jnp.sum(product, axis=0)
            gp[c, at, :] = (gated * proj[4 + c, at, :]).astype(BF16)
            gp[4 + c, at, :] = (gated * proj[c, at, :]).astype(BF16)

    for i in range(6):
        part_q[2 * chunks + i] = times(nt[...], gp[i]).astype(BF16).reshape(part_q.shape[1:])
        quads.run1(2 * chunks + i, i % 2 == 0)
    for i in range(6):
        slot = i % 4
        win(i, slot).wait()
        for q in range(cols):
            span = slice(q * WIDE, (q + 1) * WIDE)
            term = times_t(gp[i], wbuf[slot, span, :])
            if i == 0:
                out_acc[:, span] = term
            else:
                out_acc[:, span] += term
        if i + 4 < 6:
            win(i + 4, slot).start()
    for q in range(cols):
        exchange(1, sb, rb, q).wait_send()
    for q in range(cols):
        exchange(2, sa, ra, q).wait_recv()
    for q in range(cols):
        span = slice(q * WIDE, (q + 1) * WIDE)
        sb[:, span] = out_acc[:, span].astype(BF16)
        exchange(3, sb, rb, q).start()

    for q in range(cols):
        exchange(2, sa, ra, q).wait_send()

    @pl.loop(0, rows // 16)
    def _(r):
        at = pl.ds(pl.multiple_of(r * 16, 16), 16)
        sa[at, :] = (mid[at, :] + (sa[at, :].astype(F32) + ra[at, :].astype(F32))).astype(BF16)

    out_copy = pltpu.make_async_copy(sa, out_hbm, load_sem.at[4])
    out_copy.start()

    for q in range(cols):
        exchange(3, sb, rb, q).wait_recv()

    @pl.loop(0, rows // 16)
    def _(r):
        at = pl.ds(pl.multiple_of(r * 16, 16), 16)
        grad = sb[at, :].astype(F32) + rb[at, :].astype(F32)
        stream = og[at, :].astype(F32)
        scale = lax.rsqrt(mean_of(stream * stream) + EPSILON)
        weighted = grad * gain_mix[...].astype(F32)
        sums[0] += fold(grad * stream * scale)
        gn_acc[at, :] += scale * weighted - stream * (scale * scale * scale) * mean_of(weighted * stream)

    in_copy = pltpu.make_async_copy(gn_acc, in_grad_hbm, load_sem.at[5])
    in_copy.start()

    lines = [jnp.sum(sums[0], axis=0, keepdims=True), jnp.sum(sums[1], axis=0, keepdims=True)]
    tap_lines = [[jnp.sum(taps_sum[c, k], axis=0, keepdims=True) for c in range(2)] for k in range(3)]
    for k in range(8):
        piece = [line[:, k * 128 : (k + 1) * 128] for line in lines]
        group = k // 2
        start = (group % 2) * 128
        piece += [tap_lines[t][group // 2][:, start : start + 128] for t in range(3)]
        tile = jnp.concatenate(piece + [jnp.zeros((3, 128), F32)], axis=0)
        for side in range(2):
            part_s[0, k // 2, k % 2, side] = tile
    smalls.run1(0, True)

    todo = []
    for j in range(5, chunks):
        todo += [(quads, j, True), (quads, chunks + j, False)]
    early = [(quads, j, True) for j in range(5)] + [(quads, chunks + j, False) for j in range(5)]
    todo += [(downs, q, q % 2 == 0) for q in range(cols)]
    todo += [(smalls, 0, True)]
    todo += [(outs, q, q % 2 == 1) for q in range(cols)]
    todo += [(quads, 2 * chunks + i, i % 2 == 0) for i in range(6)]
    staging = {id(quads): stage_q, id(downs): stage_d, id(outs): stage_o, id(smalls): stage_s}

    def target(group, u):
        if group is quads:
            if u < chunks:
                return gate_hbm.at[:, pl.ds(u * WIDE, WIDE)]
            if u < 2 * chunks:
                return up_hbm.at[:, pl.ds((u - chunks) * WIDE, WIDE)]
            i = u - 2 * chunks
            return in_hbm.at[i // 2, :, pl.ds((i % 2) * WIDE, WIDE)]
        if group is downs:
            return down_hbm.at[:, pl.ds(u * WIDE, WIDE)]
        if group is outs:
            return outw_hbm.at[:, pl.ds(u * WIDE, WIDE)]
        return small_hbm

    stores = []

    def finish(group, u, x_first):
        spot = staging[id(group)].at[u]
        spot[...] = group.run4(u, x_first)
        copy = pltpu.make_async_copy(spot, target(group, u), store_sem.at[group.base + u])
        copy.start()
        stores.append(copy)

    pairs = [early[k] for j in range(5) for k in (j, 5 + j)]
    queue2 = list(todo)
    queue3 = pairs + todo
    queue4 = pairs + todo
    LAG = 4
    done3 = done4 = 0
    for step in range(len(queue3) + LAG):
        if step < len(queue2):
            group, u, x_first = queue2[step]
            group.run2(u, x_first)
        if step < len(queue3):
            group, u, x_first = queue3[step]
            group.run3(u, x_first)
        if step >= LAG:
            group, u, x_first = queue4[step - LAG]
            finish(group, u, x_first)
    for group, u, x_first in queue4:
        group.drain(u, x_first)
    for copy in stores:
        copy.wait()
    out_copy.wait()
    in_copy.wait()
    for q in range(cols):
        exchange(3, sb, rb, q).wait_send()
    for c in range(2):

        @pl.when(me < last)
        def _():
            halo_fwd(c).wait_send()

        @pl.when(me > 0)
        def _():
            halo_back(c).wait_send()


def whole_block(inputs, out_grad, mix_gain, in_weight, conv_weight, out_weight, ffn_gain, gate_weight, up_weight, down_weight):
    rows, width = inputs.shape[1:]
    hidden = gate_weight.shape[2]
    channels = out_weight.shape[1]
    chunks = hidden // WIDE
    quads, cols = 2 * chunks + 3 * channels // WIDE, width // WIDE
    n = lax.axis_size("seq")

    def buffers(count, length, lanes, kind):
        return [
            pltpu.VMEM((count, 4, 2, 2, length, lanes), kind),
            pltpu.VMEM((count, 4, 2, length, lanes), kind),
            pltpu.VMEM((count, 4, length, lanes), kind),
            pltpu.VMEM((count, 3, length, lanes), kind),
        ]

    lq, ld, lo = width // n, hidden // n, channels // n
    total = quads + 2 * cols + 1
    hbm = pl.BlockSpec(memory_space=pl.ANY)
    vmem = pl.BlockSpec(memory_space=pltpu.VMEM)
    big = pltpu.VMEM((rows, width), BF16)
    wide = pltpu.VMEM((rows, width), F32)
    results = pl.pallas_call(
        block_kernel,
        out_shape=[
            jax.ShapeDtypeStruct((rows, width), BF16),
            jax.ShapeDtypeStruct((rows, width), F32),
            jax.ShapeDtypeStruct((lq, hidden), F32),
            jax.ShapeDtypeStruct((lq, hidden), F32),
            jax.ShapeDtypeStruct((ld, width), F32),
            jax.ShapeDtypeStruct((3, lq, channels), F32),
            jax.ShapeDtypeStruct((lo, width), F32),
            jax.ShapeDtypeStruct((8, 128), F32),
        ],
        in_specs=[hbm] * 7 + [vmem] * 3,
        out_specs=[hbm] * 8,
        scratch_shapes=[
            big, big, pltpu.VMEM((width, rows), BF16), wide,
            pltpu.VMEM((6, rows, WIDE), F32), pltpu.VMEM((2, rows + 8, WIDE), F32), pltpu.VMEM((2, rows + 8, WIDE), F32),
            pltpu.VMEM((2, rows, WIDE), BF16), pltpu.VMEM((channels, width), BF16),
            pltpu.VMEM((4, width, WIDE), BF16), pltpu.VMEM((2, WIDE, width), BF16), wide, wide,
            big, big, big, big, pltpu.VMEM((6, rows, WIDE), BF16), pltpu.VMEM((3, rows, WIDE), F32),
            pltpu.VMEM((2, 8, width), F32), pltpu.VMEM((2, 3, 8, WIDE), F32),
            *buffers(quads, lq, WIDE, BF16), *buffers(cols, ld, WIDE, BF16),
            *buffers(cols, lo, WIDE, BF16), *buffers(1, 8, 128, F32),
            pltpu.VMEM((quads, lq, WIDE), F32), pltpu.VMEM((cols, ld, WIDE), F32),
            pltpu.VMEM((cols, lo, WIDE), F32), pltpu.VMEM((1, 8, 128), F32),
            *[pltpu.SemaphoreType.DMA((total,))] * 4, *[pltpu.SemaphoreType.DMA((total, 3))] * 2,
            pltpu.SemaphoreType.DMA((6,)), pltpu.SemaphoreType.DMA((4,)), pltpu.SemaphoreType.DMA((2,)),
            pltpu.SemaphoreType.DMA((4, cols)), pltpu.SemaphoreType.DMA((4, cols)),
            pltpu.SemaphoreType.DMA((4,)), pltpu.SemaphoreType.DMA((4,)), pltpu.SemaphoreType.DMA((total,)),
        ],
        compiler_params=pltpu.CompilerParams(collective_id=0, has_side_effects=True, vmem_limit_bytes=VMEM_BYTES),
    )(
        inputs[0], out_grad[0], in_weight.reshape(width, 3 * channels), out_weight[0],
        gate_weight[0], up_weight[0], down_weight[0], mix_gain, conv_weight[0], ffn_gain,
    )
    output, in_grad, gate_s, up_s, down_s, in_s, out_s, small = results
    index = lax.axis_index("seq")
    y, x = (index // 2) % 2, index % 2
    gains = lax.dynamic_slice(small, (0, x * 64), (2, 64))
    conv_s = lax.dynamic_slice(small, (2, y * 64 + x * 32), (3, 32))
    return (
        output[None], in_grad[None], gains[0:1], in_s.transpose(1, 0, 2)[None], conv_s[None],
        out_s[None], gains[1:2], gate_s[None], up_s[None], down_s[None],
    )


def inverse_rms(stream):
    return lax.rsqrt(jnp.mean(stream * stream, axis=-1, keepdims=True) + EPSILON)


def norm_back(grad_normed, stream, inv_scale, gain_vec):
    weighted = grad_normed * gain_vec
    gain_grad = jnp.sum(grad_normed * stream * inv_scale, axis=(0, 1))
    cubed = inv_scale * inv_scale * inv_scale
    grad_before = inv_scale * weighted - stream * cubed * jnp.mean(
        weighted * stream, axis=-1, keepdims=True
    )
    return (gain_grad, grad_before)


def forward_block(stream, weights):
    gain_mix, weight_in, weight_conv, weight_out, gain_ffn, weight_gate, weight_up, weight_down = (
        weights
    )
    seq_count, rows_in, model_width = stream.shape
    channels = weight_in.shape[-1]
    hidden = weight_gate.shape[-1]
    scale_mix = inverse_rms(stream)
    normed_mix = (stream * scale_mix * gain_mix.astype(jnp.float32)).astype(jnp.bfloat16)
    projected = jnp.dot(
        normed_mix.reshape(-1, model_width),
        weight_in.reshape(model_width, 3 * channels),
        preferred_element_type=jnp.float32,
    )
    projected = projected.reshape(seq_count, rows_in, 3, channels)
    gated_in = projected[:, :, 0] * projected[:, :, 2]
    carried = shifted(gated_in[:, -2:], "seq", 1)
    extended = jnp.concatenate([carried, gated_in], axis=1)
    out_rows = extended.shape[1] - 2
    kernel = weight_conv.astype(jnp.float32)
    convolved = (
        kernel[0] * extended[:, :out_rows]
        + kernel[1] * extended[:, 1 : out_rows + 1]
        + kernel[2] * extended[:, 2:]
    )
    mixed_out = (projected[:, -out_rows:, 1] * convolved).astype(jnp.bfloat16)
    partial_out = jnp.dot(
        mixed_out.reshape(-1, channels), weight_out, preferred_element_type=jnp.float32
    )
    middle = stream + pair_sum(partial_out).reshape(seq_count, out_rows, model_width)
    scale_ffn = inverse_rms(middle)
    normed_ffn = (middle * scale_ffn * gain_ffn.astype(jnp.float32)).astype(jnp.bfloat16)
    flat_ffn = normed_ffn.reshape(-1, model_width)
    gate_pre = jnp.dot(flat_ffn, weight_gate, preferred_element_type=jnp.float32)
    up_pre = jnp.dot(flat_ffn, weight_up, preferred_element_type=jnp.float32)
    activated = (jax.nn.silu(gate_pre) * up_pre).astype(jnp.bfloat16)
    partial_ffn = jnp.dot(activated, weight_down, preferred_element_type=jnp.float32)
    result = middle + pair_sum_low(partial_ffn).reshape(seq_count, out_rows, model_width)
    stored = (
        stream,
        scale_mix,
        normed_mix,
        projected,
        extended,
        convolved,
        mixed_out,
        middle,
        scale_ffn,
        normed_ffn,
        gate_pre.reshape(seq_count, out_rows, hidden),
        up_pre.reshape(seq_count, out_rows, hidden),
        activated.reshape(seq_count, out_rows, hidden),
    )
    return (result, stored)


def backward_ffn(grad_stream, stored, weights):
    gain_mix, weight_in, weight_conv, weight_out, gain_ffn, weight_gate, weight_up, weight_down = (
        weights
    )
    (
        block_in,
        scale_mix,
        normed_mix,
        projected,
        extended,
        convolved,
        mixed_out,
        middle,
        scale_ffn,
        normed_ffn,
        gate_pre,
        up_pre,
        activated,
    ) = stored
    seq_count, own_len, model_width = grad_stream.shape
    hidden = weight_gate.shape[-1]
    rounded = grad_stream.astype(jnp.bfloat16).reshape(-1, model_width)
    grad_hidden = jnp.einsum("nd,fd->nf", rounded, weight_down, preferred_element_type=jnp.float32)
    down_grad = jnp.einsum(
        "nf,nd->fd", activated.reshape(-1, hidden), rounded, preferred_element_type=jnp.float32
    )
    gate_flat = gate_pre.reshape(-1, hidden)
    up_flat = up_pre.reshape(-1, hidden)
    sigmoid_gate = jax.nn.sigmoid(gate_flat)
    grad_gate = (
        grad_hidden * up_flat * sigmoid_gate * (1.0 + gate_flat * (1.0 - sigmoid_gate))
    ).astype(jnp.bfloat16)
    grad_up = (grad_hidden * gate_flat * sigmoid_gate).astype(jnp.bfloat16)
    flat_ffn = normed_ffn.reshape(-1, model_width)
    gate_grad = jnp.einsum("nd,nf->df", flat_ffn, grad_gate, preferred_element_type=jnp.float32)
    up_grad = jnp.einsum("nd,nf->df", flat_ffn, grad_up, preferred_element_type=jnp.float32)
    partial_ffn = jnp.einsum(
        "nf,df->nd", grad_gate, weight_gate, preferred_element_type=jnp.float32
    )
    partial_ffn = partial_ffn + jnp.einsum(
        "nf,df->nd", grad_up, weight_up, preferred_element_type=jnp.float32
    )
    grad_normed = pair_sum(partial_ffn).reshape(seq_count, own_len, model_width)
    ffn_gain_grad, grad_middle = norm_back(
        grad_normed, middle, scale_ffn, gain_ffn.astype(jnp.float32)
    )
    grad_middle = grad_stream + grad_middle
    return (grad_middle, (ffn_gain_grad, gate_grad, up_grad, down_grad))


def backward_mixer(grad_middle, stored, weights):
    gain_mix, weight_in, weight_conv, weight_out, gain_ffn, weight_gate, weight_up, weight_down = (
        weights
    )
    (
        block_in,
        scale_mix,
        normed_mix,
        projected,
        extended,
        convolved,
        mixed_out,
        middle,
        scale_ffn,
        normed_ffn,
        gate_pre,
        up_pre,
        activated,
    ) = stored
    seq_count, own_len, model_width = grad_middle.shape
    channels = weight_out.shape[0]
    rounded_mid = grad_middle.astype(jnp.bfloat16).reshape(-1, model_width)
    grad_mixed = jnp.einsum(
        "nd,cd->nc", rounded_mid, weight_out, preferred_element_type=jnp.float32
    )
    grad_mixed = grad_mixed.reshape(seq_count, own_len, channels)
    out_grad_w = jnp.einsum(
        "nc,nd->cd",
        mixed_out.reshape(-1, channels),
        rounded_mid,
        preferred_element_type=jnp.float32,
    )
    grad_conv = grad_mixed * projected[:, :, 1]
    grad_second = grad_mixed * convolved
    following = shifted(grad_conv[:, :2], "seq", -1)
    ext_grad = jnp.concatenate([grad_conv, following], axis=1)
    kernel = weight_conv.astype(jnp.float32)
    grad_gated = (
        kernel[0] * ext_grad[:, 2:] + kernel[1] * ext_grad[:, 1:-1] + kernel[2] * ext_grad[:, :-2]
    )
    conv_grad = jnp.stack(
        [
            jnp.sum(grad_conv * extended[:, offset : offset + own_len], axis=(0, 1))
            for offset in range(3)
        ]
    )
    grad_proj = jnp.stack(
        [grad_gated * projected[:, :, 2], grad_second, grad_gated * projected[:, :, 0]], axis=2
    )
    grad_proj = grad_proj.astype(jnp.bfloat16).reshape(-1, 3 * channels)
    in_grad_w = jnp.einsum(
        "nd,nk->dk",
        normed_mix.reshape(-1, model_width),
        grad_proj,
        preferred_element_type=jnp.float32,
    )
    in_grad_w = in_grad_w.reshape(model_width, 3, channels)
    partial_mix = jnp.einsum(
        "nk,dk->nd",
        grad_proj,
        weight_in.reshape(model_width, 3 * channels),
        preferred_element_type=jnp.float32,
    )
    grad_normed_mix = (
        pair_sum_low(partial_mix)
        .reshape(seq_count, own_len, model_width)
    )
    mix_gain_grad, grad_input = norm_back(
        grad_normed_mix, block_in, scale_mix, gain_mix.astype(jnp.float32)
    )
    grad_input = grad_middle + grad_input
    return (grad_input, (mix_gain_grad, in_grad_w, conv_grad, out_grad_w))


def local(
    inputs,
    out_grad,
    mix_gain,
    in_weight,
    conv_weight,
    out_weight,
    ffn_gain,
    gate_weight,
    up_weight,
    down_weight,
):
    if lax.axis_size("seq") == 16:
        return whole_block(
            inputs, out_grad, mix_gain, in_weight, conv_weight, out_weight, ffn_gain, gate_weight, up_weight, down_weight
        )
    layer_count = mix_gain.shape[0]

    def weights_of(number):
        return (
            mix_gain[number],
            in_weight[number],
            conv_weight[number],
            out_weight[number],
            ffn_gain[number],
            gate_weight[number],
            up_weight[number],
            down_weight[number],
        )

    stream = inputs.astype(jnp.float32)
    number = 0
    stream, stored = forward_block(stream, weights_of(number))
    stored_all = [stored]
    output = stream.astype(jnp.bfloat16)
    grad_stream = out_grad.astype(jnp.float32)
    ffn_parts = [None] * layer_count
    mixer_parts = [None] * layer_count
    for number in reversed(range(layer_count)):
        grad_middle, ffn_terms = backward_ffn(grad_stream, stored_all[number], weights_of(number))
        ffn_parts[number] = ffn_terms
        grad_stream, mixer_terms = backward_mixer(
            grad_middle, stored_all[number], weights_of(number)
        )
        mixer_parts[number] = mixer_terms
    joined = tuple(mixer_parts[0]) + tuple(ffn_parts[0])
    mix_gain_g, in_g, conv_g, out_g, ffn_gain_g, gate_g, up_g, down_g = joined
    n = lax.axis_size("seq")
    down_s = scatter_sum(down_g.astype(jnp.bfloat16), (0, 1, 2))
    gate_s = scatter_sum(gate_g.astype(jnp.bfloat16), (2, 1, 0))
    up_s = scatter_sum(up_g.astype(jnp.bfloat16), (1, 2, 0))
    out_s = scatter_sum(out_g.astype(jnp.bfloat16), (1, 2, 0))
    in_s = scatter_sum(in_g.astype(jnp.bfloat16), (2, 1, 0))
    taps, channels = conv_g.shape
    small = jnp.concatenate(
        [
            mix_gain_g.reshape(n, -1),
            ffn_gain_g.reshape(n, -1),
            conv_g.reshape(taps, n, -1).swapaxes(0, 1).reshape(n, -1),
        ],
        axis=1,
    )
    small = scatter_sum(small, (2, 1, 0), jnp.float32).reshape(-1)
    gain_len = mix_gain_g.shape[0] // n
    return (
        output,
        grad_stream,
        small[:gain_len][None],
        in_s[None],
        small[2 * gain_len :].reshape(1, taps, channels // n),
        out_s[None],
        small[gain_len : 2 * gain_len][None],
        gate_s[None],
        up_s[None],
        down_s[None],
    )


def solution(mesh):
    in_specs = (
        P(None, "seq", None),
        P(None, "seq", None),
        P(),
        P(None, None, None, "tensor"),
        P(None, None, "tensor"),
        P(None, "tensor", None),
        P(),
        P(None, None, "tensor"),
        P(None, None, "tensor"),
        P(None, "tensor", None),
    )
    out_specs = (
        P(None, "seq", None),
        P(None, "seq", None),
        P(None, "seq"),
        P(None, "seq", None, "tensor"),
        P(None, None, ("tensor", "seq")),
        P(None, ("tensor", "seq"), None),
        P(None, "seq"),
        P(None, "seq", "tensor"),
        P(None, "seq", "tensor"),
        P(None, ("tensor", "seq"), None),
    )
    return jax.shard_map(local, mesh=mesh, in_specs=in_specs, out_specs=out_specs, check_vma=False)
```

```python
import jax
import jax.numpy as jnp
from jax import lax
from jax.experimental import pallas as pl
from jax.experimental.pallas import tpu as pltpu
from jax.sharding import PartitionSpec as P

EPSILON = 1e-05


def shifted(block, axis, distance):
    devices = range(lax.axis_size(axis))
    route = [(i - distance, i) for i in devices if i - distance in devices]
    return lax.ppermute(block, axis, route)


DIMS = {16: (4, 2, 2), 64: (4, 4, 4)}


def seq_dims():
    n = lax.axis_size("seq")
    return DIMS.get(n, (n,))


def pair_sum(part):
    return part + lax.ppermute(part, "tensor", [(0, 1), (1, 0)])


def pair_sum_low(part):
    low = lax.optimization_barrier(part.astype(jnp.bfloat16))
    other = lax.ppermute(low, "tensor", [(0, 1), (1, 0)])
    return low.astype(jnp.float32) + other.astype(jnp.float32)


def hop(block, dims, dim, step, spots):
    n = lax.axis_size("seq")
    stride = 1
    for size in dims[dim + 1 :]:
        stride *= size
    route = [(i, i + step * stride) for i in range(n) if (i // stride) % dims[dim] in spots]
    return lax.ppermute(block, "seq", route)


def scatter_sum(whole, order, wire=jnp.bfloat16):
    dims = seq_dims()
    rest = whole.shape[1:]
    rows = whole.shape[0] // lax.axis_size("seq")
    index = lax.axis_index("seq")
    spot = []
    for size in reversed(dims):
        spot.insert(0, index % size)
        index = index // size
    parts = [(whole.reshape(dims + (rows,) + rest), list(range(len(dims))))]

    def pick(part, dim, at):
        array, left = part
        axis = left.index(dim)
        return lax.dynamic_index_in_dim(array, at, axis, keepdims=False)

    def total(parts, dim, at):
        return sum(pick(part, dim, at).astype(jnp.float32) for part in parts)

    for dim in order:
        size = dims[dim]
        here = spot[dim]
        left = [d for d in parts[0][1] if d != dim]
        if size == 2:
            sent = total(parts, dim, 1 - here).astype(wire)
            n = lax.axis_size("seq")
            stride = 1
            for other in dims[dim + 1 :]:
                stride *= other
            got = [lax.ppermute(sent, "seq", [(i, i + stride * (1 - 2 * ((i // stride) % 2))) for i in range(n)])]
        else:
            got = []
            for step in (1, -1):
                carried = None
                for distance in range(size - 1, 0, -1):
                    at = jnp.clip(here + step * distance, 0, size - 1)
                    sent = total(parts, dim, at)
                    if carried is not None:
                        sent = sent + carried.astype(jnp.float32)
                    spots = [c for c in range(size) if 0 <= c + step * distance < size]
                    carried = hop(sent.astype(wire), dims, dim, step, spots)
                got.append(carried)
        parts = [(pick(part, dim, here), left) for part in parts] + [(block, left) for block in got]
    return sum(part.astype(jnp.float32) for part, _ in parts)


MESH = pl.DeviceIdType.MESH
VMEM_BYTES = 67043328
F32, BF16 = jnp.float32, jnp.bfloat16
WIDE = 256


def times(a, b):
    return jnp.dot(a, b, preferred_element_type=F32)


def times_t(a, b):
    return lax.dot_general(a, b, (((1,), (1,)), ((), ())), preferred_element_type=F32)


def device_of(z, y, x):
    return {"seq": z * 4 + y * 2 + x}


class Scatter:
    def __init__(self, base, part, first, second, third, sems):
        self.base, self.part = base, part
        self.first, self.second, self.third = first, second, third
        self.send1, self.recv1, self.send2, self.recv2, self.send3, self.recv3 = sems
        me = lax.axis_index("seq")
        self.z, self.y, self.x = me // 4, (me // 2) % 2, me % 2

    def stage1(self, u, x_first):
        z, y, x = self.z, self.y, self.x
        if x_first:
            source, target = self.part(u).at[:, :, 1 - x], device_of(z, y, 1 - x)
        else:
            source, target = self.part(u).at[:, 1 - y], device_of(z, 1 - y, x)
        k = self.base + u
        return pltpu.make_async_remote_copy(
            source, self.first.at[u], self.send1.at[k], self.recv1.at[k], device_id=target, device_id_type=MESH
        )

    def stage2(self, u, x_first):
        z, y, x = self.z, self.y, self.x
        if x_first:
            source, target = self.first.at[u, :, 1 - y], device_of(z, 1 - y, x)
        else:
            source, target = self.first.at[u, :, 1 - x], device_of(z, y, 1 - x)
        k = self.base + u
        return pltpu.make_async_remote_copy(
            source, self.second.at[u], self.send2.at[k], self.recv2.at[k], device_id=target, device_id_type=MESH
        )

    def stage3(self, u, d):
        other = (self.z + d) % 4
        k = self.base + u
        return pltpu.make_async_remote_copy(
            self.second.at[u, other], self.third.at[u, d - 1], self.send3.at[k, d - 1], self.recv3.at[k, d - 1],
            device_id=device_of(other, self.y, self.x), device_id_type=MESH,
        )

    def run1(self, u, x_first):
        self.stage1(u, x_first).start()

    def run2(self, u, x_first):
        y, x = self.y, self.x
        self.stage1(u, x_first).wait_recv()

        @pl.loop(0, 4)
        def _(at):
            if x_first:
                mine, spot = self.part(u).at[at, 1 - y, x], self.first.at[u, at, 1 - y]
            else:
                mine, spot = self.part(u).at[at, y, 1 - x], self.first.at[u, at, 1 - x]
            spot[...] = (mine[...].astype(F32) + spot[...].astype(F32)).astype(spot.dtype)

        self.stage2(u, x_first).start()

    def kept(self, u, x_first, at):
        y, x = self.y, self.x
        near = self.first.at[u, at, y if x_first else x]
        return (
            self.part(u)[at, y, x].astype(F32) + near[...].astype(F32) + self.second[u, at].astype(F32)
        )

    def run3(self, u, x_first):
        self.stage2(u, x_first).wait_recv()

        @pl.loop(1, 4)
        def _(d):
            other = (self.z + d) % 4
            self.second[u, other] = self.kept(u, x_first, other).astype(self.second.dtype)

        for d in range(1, 4):
            self.stage3(u, d).start()

    def run4(self, u, x_first):
        for d in range(1, 4):
            self.stage3(u, d).wait_recv()
        total = self.kept(u, x_first, self.z)
        for d in range(1, 4):
            total = total + self.third[u, d - 1].astype(F32)
        return total

    def drain(self, u, x_first):
        self.stage1(u, x_first).wait_send()
        self.stage2(u, x_first).wait_send()
        for d in range(1, 4):
            self.stage3(u, d).wait_send()


class Halves:
    def __init__(self, part, first, third, across_send, across_recv, sems):
        self.part, self.first, self.third = part, first, third
        self.across_send, self.across_recv = across_send, across_recv
        self.send1, self.recv1, self.send3, self.recv3, self.send4, self.recv4 = sems
        me = lax.axis_index("seq")
        self.z, self.y, self.x = me // 4, (me // 2) % 2, me % 2

    def stage1(self, u):
        return pltpu.make_async_remote_copy(
            self.part(u).at[:, 1 - self.y], self.first.at[u], self.send1.at[u], self.recv1.at[u],
            device_id=device_of(self.z, 1 - self.y, self.x), device_id_type=MESH,
        )

    def stage3(self, u, d):
        other = (self.z + d) % 4
        return pltpu.make_async_remote_copy(
            self.first.at[u, other], self.third.at[u, d - 1], self.send3.at[u, d - 1], self.recv3.at[u, d - 1],
            device_id=device_of(other, self.y, self.x), device_id_type=MESH,
        )

    def stage4(self, u):
        return pltpu.make_async_remote_copy(
            self.across_send.at[u], self.across_recv.at[u], self.send4.at[u], self.recv4.at[u],
            device_id=device_of(self.z, self.y, 1 - self.x), device_id_type=MESH,
        )

    def run1(self, u):
        self.stage1(u).start()

    def run2(self, u):
        self.stage1(u).wait_recv()

        @pl.loop(0, 6)
        def _(k):
            other, side = (self.z + 1 + k // 2) % 4, k % 2
            spot = self.first.at[u, other, side]
            spot[...] = (self.part(u)[other, self.y, side].astype(F32) + spot[...].astype(F32)).astype(BF16)

        for d in range(1, 4):
            self.stage3(u, d).start()

    def total(self, u, side):
        value = self.part(u)[self.z, self.y, side].astype(F32) + self.first[u, self.z, side].astype(F32)
        for d in range(1, 4):
            value = value + self.third[u, d - 1, side].astype(F32)
        return value

    def run3(self, u):
        for d in range(1, 4):
            self.stage3(u, d).wait_recv()
        self.across_send[u] = self.total(u, 1 - self.x).astype(BF16)
        self.stage4(u).start()
        return self.total(u, self.x)

    def run4(self, u):
        self.stage4(u).wait_recv()
        return self.across_recv[u].astype(F32)

    def drain(self, u):
        self.stage1(u).wait_send()
        for d in range(1, 4):
            self.stage3(u, d).wait_send()
        self.stage4(u).wait_send()


class Line:
    def __init__(self, part, first, chain, extra, across_send, across_recv, sems):
        self.part, self.first, self.chain, self.extra = part, first, chain, extra
        self.across_send, self.across_recv = across_send, across_recv
        (self.send1, self.recv1, self.send2, self.recv2, self.send3, self.recv3, self.send4, self.recv4) = sems
        me = lax.axis_index("seq")
        self.z, self.y, self.x = me // 4, (me // 2) % 2, me % 2
        self.place = self.z + self.x * (3 - 2 * self.z)
        self.nearer = (self.z + 3 + 2 * self.x) % 4
        self.farther = (self.z + 1 + 2 * self.x) % 4
        self.block0, self.block1 = self.x, 1 - self.x

    def stage1(self, q):
        return pltpu.make_async_remote_copy(
            self.part.at[q, :, 1 - self.y], self.first.at[q], self.send1.at[q], self.recv1.at[q],
            device_id=device_of(self.z, 1 - self.y, self.x), device_id_type=MESH,
        )

    def both(self, q):
        return pltpu.make_async_remote_copy(
            self.first.at[q], self.chain.at[q], self.send2.at[q], self.recv2.at[q],
            device_id=device_of(self.nearer, self.y, self.x), device_id_type=MESH,
        )

    def inward(self, q):
        return pltpu.make_async_remote_copy(
            self.first.at[q, self.block0], self.extra.at[q], self.send3.at[q], self.recv3.at[q],
            device_id=device_of(self.nearer, self.y, self.x), device_id_type=MESH,
        )

    def outward(self, q):
        return pltpu.make_async_remote_copy(
            self.first.at[q, self.block1], self.extra.at[q], self.send3.at[q], self.recv3.at[q],
            device_id=device_of(self.farther, self.y, self.x), device_id_type=MESH,
        )

    def stage4(self, q):
        return pltpu.make_async_remote_copy(
            self.across_send.at[q], self.across_recv.at[q], self.send4.at[q], self.recv4.at[q],
            device_id=device_of(self.z, self.y, 1 - self.x), device_id_type=MESH,
        )

    def run1(self, q):
        self.stage1(q).start()

    def add(self, q, block, other):
        @pl.loop(0, 2)
        def _(side):
            spot = self.first.at[q, block, side]
            spot[...] = (spot[...].astype(F32) + other[block, side].astype(F32)).astype(BF16)

    def run2(self, q):
        self.stage1(q).wait_recv()
        for block in range(2):
            self.add(q, block, self.part.at[q, :, self.y])

        @pl.when(self.place == 3)
        def _():
            self.both(q).start()

        @pl.when(self.place == 0)
        def _():
            self.outward(q).start()

    def run3(self, q):
        @pl.when(self.place == 2)
        def _():
            self.both(q).wait_recv()
            for block in range(2):
                self.add(q, block, self.chain.at[q])
            self.both(q).start()

    def run4(self, q):
        @pl.when(self.place == 1)
        def _():
            self.both(q).wait_recv()
            for block in range(2):
                self.add(q, block, self.chain.at[q])
            self.inward(q).start()

    def run5(self, q, spot):
        @pl.when(self.place < 2)
        def _():
            self.inward(q).wait_recv()
            block = (self.place + self.x) % 2
            far = self.first[q, block, 1 - self.x].astype(F32) + self.extra[q, 1 - self.x].astype(F32)
            self.across_send[q] = far.astype(BF16)
            self.stage4(q).start()
            spot[...] = self.first[q, block, self.x].astype(F32) + self.extra[q, self.x].astype(F32)

    def run6(self, q, spot):
        @pl.when(self.place >= 2)
        def _():
            self.stage4(q).wait_recv()
            spot[...] = self.across_recv[q].astype(F32)

    def drain(self, q):
        self.stage1(q).wait_send()

        @pl.when(self.place >= 2)
        def _():
            self.both(q).wait_send()

        @pl.when(self.place < 2)
        def _():
            self.inward(q).wait_send()
            self.stage4(q).wait_send()


def block_kernel(
    x_hbm, og_hbm, win_hbm, wout_hbm, wg_hbm, wu_hbm, wd_hbm, gain_mix, taps, gain_ffn,
    out_hbm, in_grad_hbm, gate_hbm, up_hbm, down_hbm, in_hbm, outw_hbm, small_hbm,
    xb, og, nf, nt, act, gg, gu, mid, gm, gno, proj, gext, gcon, mixed, wout, wg, wu, wd, hid,
    sa, ra, gnp, gnr, gnx, outp, outr, outx, sums, taps_sum,
    part_g, part_u, first_g, third_g, asend_g, arecv_g,
    part_d, first_d, chain_d, extra_d, asend_d, arecv_d,
    first_i, second_i, third_i, first_o, second_o, third_o,
    part_s, first_s, second_s, third_s, recv_s,
    stage_g, stage_d, stage_i, stage_o, stage_s,
    gs1, gr1, gs3, gr3, gs4, gr4, ds1, dr1, ds2, dr2, ds3, dr3, ds4, dr4,
    send1, recv1, send2, recv2, send3, recv3,
    load_sem, lsend, lrecv, mid_send, mid_recv, halo_send, halo_recv, g_sem, d_sem, m_sem,
):
    rows, width = x_hbm.shape
    half = rows // 2
    me = lax.axis_index("seq")
    last = lax.axis_size("seq") - 1
    core = lax.axis_index("tensor")
    z, y, x = me // 4, (me // 2) % 2, me % 2
    mate, across = {"tensor": 1 - core}, device_of(z, y, 1 - x)
    share = wd.shape[0]
    cols = width // WIDE
    GROUP = 384
    groups = share // GROUP
    spans = ((0, 512), (512, share - 512))

    def rows_of(block):
        return pl.ds(pl.multiple_of(block * half, half), half)

    mine, theirs = rows_of(core), rows_of(1 - core)
    mine_x, theirs_x = rows_of(2 + core), rows_of(3 - core)

    def columns(ref, start, size):
        return ref.at[:, :, :, :, pl.ds(start, size)]

    grads = Halves(
        lambda u: columns(part_g if u < groups else part_u, (u % groups) * GROUP, GROUP),
        first_g, third_g, asend_g, arecv_g, (gs1, gr1, gs3, gr3, gs4, gr4),
    )
    downs = Line(part_d, first_d, chain_d, extra_d, asend_d, arecv_d, (ds1, dr1, ds2, dr2, ds3, dr3, ds4, dr4))
    sems = (send1, recv1, send2, recv2, send3, recv3)
    ins = Scatter(0, lambda u: columns(gg if u < 4 else gu, (u % 4) * WIDE, WIDE), first_i, second_i, third_i, sems)
    outs = Scatter(6, lambda u: act.at[:, :, :, 0:32, pl.ds(u * WIDE, WIDE)], first_o, second_o, third_o, sems)
    smalls = Scatter(10, lambda u: part_s, first_s, second_s, third_s, sems)

    def load(index, source, target):
        return pltpu.make_async_copy(source, target, load_sem.at[index])

    def send(index, source, target, device):
        return pltpu.make_async_remote_copy(
            source, target, lsend.at[index], lrecv.at[index], device_id=device, device_id_type=MESH
        )

    x_og = send(0, og_hbm.at[mine], og.at[mine_x], across)
    m_og = send(1, og.at[mine_x], og.at[mine_x], mate)
    m_nf = send(2, nf.at[mine], nf.at[mine], mate)
    x_nf = send(3, nf.at[mine], nf.at[mine_x], across)
    m_nfx = send(4, nf.at[mine_x], nf.at[mine_x], mate)
    m_gn0 = send(5, gnp.at[1 - core], gnr.at[0], mate)
    m_gn1 = send(6, gnp.at[3 - core], gnr.at[1], mate)
    x_gn = send(7, gnp.at[2 + core], gnx, across)
    m_out0 = send(8, outp.at[1 - core], outr.at[0], mate)
    m_out1 = send(9, outp.at[3 - core], outr.at[1], mate)
    x_out = send(10, outp.at[2 + core], outx, across)
    m_rmid = send(11, xb.at[mine], xb.at[mine], mate)
    m_in = send(12, gm, in_grad_hbm.at[mine], mate)
    m_small = send(14, stage_s, recv_s, mate)

    def m_mid(turn, q):
        span = pl.ds(q * WIDE, WIDE)
        return pltpu.make_async_remote_copy(
            sa.at[:, span], ra.at[:, span], mid_send.at[turn, q], mid_recv.at[turn, q], device_id=mate, device_id_type=MESH
        )

    def win_loads():
        return (
            load(2, win_hbm.at[:, pl.ds(0, 1024)], wg.at[:, pl.ds(0, 1024)]),
            load(3, win_hbm.at[:, pl.ds(1024, 512)], wu.at[:, pl.ds(0, 512)]),
        )

    first_column = pl.multiple_of(x * share, 128)
    gate_load = load(4, wg_hbm.at[:, pl.ds(first_column, share)], wg)
    up_load = load(5, wu_hbm.at[:, pl.ds(first_column, share)], wu)
    down_load = load(6, wd_hbm.at[pl.ds(first_column, share)], wd)

    load(0, x_hbm, xb).start()
    for copy in win_loads():
        copy.start()
    load(1, og_hbm, og.at[pl.ds(0, rows)]).start()
    load(7, wout_hbm, wout).start()
    down_load.start()

    barrier = pltpu.get_barrier_semaphore()
    near = [across, device_of(z, 1 - y, x), *(device_of((z + d) % 4, y, x) for d in range(1, 4))]
    near += [mate, {"seq": (me + last) % (last + 1)}, {"seq": (me + 1) % (last + 1)}]
    for target in near:
        pl.semaphore_signal(barrier, inc=1, device_id=target, device_id_type=MESH)

    def mean_of(value):
        return jnp.mean(value, axis=-1, keepdims=True)

    def fold(value):
        return value[0:8] + value[8:16]

    pl.semaphore_wait(barrier, len(near))
    x_og.start()

    load(0, x_hbm, xb).wait()

    @pl.loop(0, rows // 16, unroll=4)
    def _(r):
        at = pl.ds(pl.multiple_of(r * 16, 16), 16)
        stream = xb[at, :].astype(F32)
        scale = lax.rsqrt(mean_of(stream * stream) + EPSILON)
        nf[at, :] = (stream * scale * gain_mix[...].astype(F32)).astype(BF16)

    def halo_fwd(c):
        return pltpu.make_async_remote_copy(
            gext.at[c, pl.ds(rows, 8)], gext.at[c, pl.ds(0, 8)], halo_send.at[c], halo_recv.at[c],
            device_id={"seq": me + 1}, device_id_type=MESH,
        )

    def halo_back(c):
        return pltpu.make_async_remote_copy(
            gcon.at[c, pl.ds(0, 8)], gcon.at[c, pl.ds(rows, 8)], halo_send.at[2 + c], halo_recv.at[2 + c],
            device_id={"seq": me - 1}, device_id_type=MESH,
        )

    for copy in win_loads():
        copy.wait()
    for i in (0, 4, 1, 5, 2, 3):
        weight = wg[:, i * WIDE : (i + 1) * WIDE] if i < 4 else wu[:, (i - 4) * WIDE : (i - 3) * WIDE]
        proj[i] = times(nf[0:rows, :], weight)
        if i >= 4:
            c = i - 4

            @pl.loop(0, rows // 64, unroll=2)
            def _(r):
                at = pl.ds(pl.multiple_of(r * 64, 64), 64)
                to = pl.ds(pl.multiple_of(r * 64 + 8, 8), 64)
                gext[c, to, :] = proj[c, at, :] * proj[4 + c, at, :]

            @pl.when(me < last)
            def _():
                halo_fwd(c).start()

            @pl.when(me == 0)
            def _():
                gext[c, 0:8, :] = jnp.zeros((8, WIDE), F32)

    gate_load.start()
    up_load.start()

    def tap(k, c):
        return taps[k : k + 1, c * WIDE : (c + 1) * WIDE].astype(F32)

    def convolved(c, r):
        span = gext[c, pl.ds(pl.multiple_of(r * 64, 64), 72), :]
        return tap(0, c) * span[6:70] + tap(1, c) * span[7:71] + tap(2, c) * span[8:72]

    for c in range(2):

        @pl.when(me > 0)
        def _():
            halo_fwd(c).wait_recv()

        @pl.loop(0, rows // 64, unroll=2)
        def _(r):
            at = pl.ds(pl.multiple_of(r * 64, 64), 64)
            mixed[c, at, :] = (proj[2 + c, at, :] * convolved(c, r)).astype(BF16)

    load(7, wout_hbm, wout).wait()

    def out_part(at, q):
        span = slice(q * WIDE, (q + 1) * WIDE)
        return times(mixed[0, at, :], wout[0:WIDE, span]) + times(mixed[1, at, :], wout[WIDE : 2 * WIDE, span])

    for q in range(cols):
        sa[:, q * WIDE : (q + 1) * WIDE] = out_part(theirs, q).astype(BF16)
        m_mid(0, q).start()
    for q in range(cols):
        mid[:, q * WIDE : (q + 1) * WIDE] = out_part(mine, q)
    for q in range(cols):
        m_mid(0, q).wait_recv()

    @pl.loop(0, half // 16, unroll=4)
    def _(r):
        at = pl.ds(pl.multiple_of(r * 16, 16), 16)
        here = pl.ds(pl.multiple_of(core * half + r * 16, 16), 16)
        stream = xb[here, :].astype(F32) + (mid[at, :] + ra[at, :].astype(F32))
        mid[at, :] = stream
        scale = lax.rsqrt(mean_of(stream * stream) + EPSILON)
        nf[here, :] = (stream * scale * gain_ffn[...].astype(F32)).astype(BF16)

    m_nf.start()
    x_nf.start()

    def turn_block(block):
        nt[:, rows_of(block)] = nf[rows_of(block), :].T

    def hidden_of(block):
        at = rows_of(block)
        for start, size in spans:
            hid[0, :, 0:size] = times(nf[at, :], wg[:, start : start + size])
            hid[1, :, 0:size] = times(nf[at, :], wu[:, start : start + size])
            hid[2, :, 0:size] = times_t(og[at, :], wd[start : start + size, :])

            @pl.loop(0, half // 16, unroll=4)
            def _(r):
                line = pl.ds(pl.multiple_of(r * 16, 16), 16)
                spot = (block, r // 8, (r // 4) % 2, pl.ds(pl.multiple_of((r % 4) * 16, 16), 16), slice(start, start + size))
                gate, up, back = hid[0, line, 0:size], hid[1, line, 0:size], hid[2, line, 0:size]
                s = jax.nn.sigmoid(gate)
                silu = gate * s
                act[spot] = (silu * up).astype(BF16)
                gg[spot] = (back * up * s * (1.0 + gate * (1.0 - s))).astype(BF16)
                gu[spot] = (back * silu).astype(BF16)

    def gradient_of(block):
        for q in range(cols):
            span = slice(q * WIDE, (q + 1) * WIDE)
            gnp[block, :, span] = (
                times_t(gg[block].reshape(half, share), wg[span, :]) + times_t(gu[block].reshape(half, share), wu[span, :])
            ).astype(BF16)

    def output_of(block):
        for q in range(cols):
            span = slice(q * WIDE, (q + 1) * WIDE)
            outp[block, :, span] = times(act[block].reshape(half, share), wd[:, span]).astype(BF16)

    load(1, og_hbm, og.at[pl.ds(0, rows)]).wait()
    gate_load.wait()
    up_load.wait()
    down_load.wait()

    @pl.loop(0, 2)
    def _(i):
        @pl.when(i == 1)
        def _():
            m_nf.wait_recv()
            x_og.wait_recv()
            m_og.start()

        block = (core + i) % 2
        turn_block(block)
        hidden_of(block)

    @pl.loop(0, 2)
    def _(i):
        block = (core + 1 + i) % 2
        gradient_of(block)
        output_of(block)

        @pl.when(i == 0)
        def _():
            m_gn0.start()
            m_out0.start()

    @pl.loop(0, 2)
    def _(i):
        @pl.when(i == 0)
        def _():
            x_nf.wait_recv()
            m_nfx.start()

        @pl.when(i == 1)
        def _():
            m_og.wait_recv()
            m_nfx.wait_recv()

        block = 2 + (core + i) % 2
        turn_block(block)
        hidden_of(block)

    for copy in (m_nf, x_nf, m_nfx, m_og):
        copy.wait_send()
    tokens = 2 * rows
    pieces = [(nf, 0, 288), (nf, 288, 288), (nf, 576, 288), (nf, 864, 160), (xb, 0, 128)]

    def turn_activated():
        for piece in range(groups):
            size = min(GROUP, 2 * rows - piece * GROUP)
            turned = act[:, :, :, :, piece * GROUP : (piece + 1) * GROUP].reshape(tokens, GROUP).T
            nf[piece * GROUP : piece * GROUP + size, :] = turned[0:size]
            if size < GROUP:
                xb[0 : GROUP - size, :] = turned[size:GROUP]

    def down_part(q):
        row = 0
        for source, start, size in pieces:
            block = times(source[start : start + size, :], og[:, q * WIDE : (q + 1) * WIDE]).astype(BF16)
            at = 0
            while at < size:
                shard, offset = divmod(row + at, 144)
                count = min(144 - offset, size - at)
                part_d[q, shard // 4, (shard // 2) % 2, shard % 2, offset : offset + count, :] = block[at : at + count]
                at += count
            row += size
        if q == cols - 1:
            load(0, x_hbm, og.at[pl.ds(rows, rows)]).start()

    def hidden_part(part, source):
        for start, size in spans:

            @pl.loop(0, 4)
            def _(m):
                lhs = nt[pl.ds(pl.multiple_of(m * WIDE, WIDE), WIDE), :]
                block = times(lhs, source[:, :, :, :, start : start + size].reshape(tokens, size))
                part[m, :, :, :, start : start + size] = block.astype(BF16).reshape(2, 2, 64, size)

    def join(mine_part, other_part):
        @pl.loop(0, half // 32, unroll=2)
        def _(r):
            at = pl.ds(pl.multiple_of(r * 32, 32), 32)
            mine_part[at, :] = (mine_part[at, :].astype(F32) + other_part[at, :].astype(F32)).astype(BF16)

    def gradient_theirs():
        gradient_of(3 - core)
        m_gn1.start()

    def gradient_mine():
        gradient_of(2 + core)
        m_gn1.wait_recv()
        join(gnp.at[2 + core], gnr.at[1])
        x_gn.start()

    def output_both():
        output_of(3 - core)
        m_out1.start()
        output_of(2 + core)
        m_out1.wait_recv()
        join(outp.at[2 + core], outr.at[1])
        x_out.start()
        for copy in win_loads():
            copy.start()

    def ffn_norm():
        m_gn0.wait_recv()
        x_gn.wait_recv()
        sums[...] = jnp.zeros_like(sums)

        @pl.loop(0, half // 16, unroll=4)
        def _(r):
            at = pl.ds(pl.multiple_of(r * 16, 16), 16)
            here = pl.ds(pl.multiple_of(core * half + r * 16, 16), 16)
            grad = gnp[core, at, :].astype(F32) + gnr[0, at, :].astype(F32) + gnx[at, :].astype(F32)
            stream = mid[at, :]
            scale = lax.rsqrt(mean_of(stream * stream) + EPSILON)
            weighted = grad * gain_ffn[...].astype(F32)
            sums[1] += fold(grad * stream * scale)
            middle = og[here, :].astype(F32) + (
                scale * weighted - stream * (scale * scale * scale) * mean_of(weighted * stream)
            )
            gm[at, :] = middle
            xb[here, :] = middle.astype(BF16)

        m_rmid.start()
        load(0, x_hbm, og.at[pl.ds(rows, rows)]).wait()

        @pl.loop(0, rows // 128)
        def _(r):
            at = pl.ds(pl.multiple_of(r * 128, 128), 128)
            stream = og[pl.ds(pl.multiple_of(rows + r * 128, 128), 128), :].astype(F32)
            scale = lax.rsqrt(mean_of(stream * stream) + EPSILON)
            nt[:, at] = (stream * scale * gain_mix[...].astype(F32)).astype(BF16).T

        m_rmid.wait_recv()

    def mixer_back():
        @pl.loop(0, 2)
        def _(h):
            hid[h, :, 0 : 2 * WIDE] = times_t(xb[rows_of(h), :], wout[...])

        for c in range(2):
            span = slice(c * WIDE, (c + 1) * WIDE)

            @pl.loop(0, rows // 64, unroll=2)
            def _(r):
                at = pl.ds(pl.multiple_of(r * 64, 64), 64)
                grad = hid[r // 4, pl.ds(pl.multiple_of((r % 4) * 64, 64), 64), span]
                gcon[c, at, :] = grad * proj[2 + c, at, :]
                nf[at, (2 + c) * WIDE : (3 + c) * WIDE] = (grad * convolved(c, r)).astype(BF16)

            @pl.when(me > 0)
            def _():
                halo_back(c).start()

            @pl.when(me == last)
            def _():
                gcon[c, rows : rows + 8, :] = jnp.zeros((8, WIDE), F32)


    def in_grad_of(i):
        source = nf[0:rows, i * WIDE : (i + 1) * WIDE] if i < 4 else nf[rows : 2 * rows, (i - 4) * WIDE : (i - 3) * WIDE]
        block = times(nt[:, 0:rows], source).astype(BF16).reshape(4, 2, 2, 64, WIDE)
        columns(gg if i < 4 else gu, (i % 4) * WIDE, WIDE)[...] = block

    def gated_back(c):

        @pl.when(me < last)
        def _():
            halo_back(c).wait_recv()

        taps_sum[c] = jnp.zeros_like(taps_sum[c])

        @pl.loop(0, rows // 64, unroll=2)
        def _(r):
            at = pl.ds(pl.multiple_of(r * 64, 64), 64)
            ahead = gcon[c, pl.ds(pl.multiple_of(r * 64, 64), 72), :]
            behind = gext[c, pl.ds(pl.multiple_of(r * 64, 64), 72), :]
            grad = ahead[0:64]
            gated = tap(0, c) * ahead[2:66] + tap(1, c) * ahead[1:65] + tap(2, c) * grad
            for k in range(3):
                product = (grad * behind[6 + k : 70 + k]).reshape(8, 8, WIDE)
                taps_sum[c, k] += jnp.sum(product, axis=0)
            nf[at, c * WIDE : (c + 1) * WIDE] = (gated * proj[4 + c, at, :]).astype(BF16)
            nf[pl.ds(pl.multiple_of(rows + r * 64, 64), 64), c * WIDE : (c + 1) * WIDE] = (
                gated * proj[c, at, :]
            ).astype(BF16)

    def out_grad_of(c):
        mixed_t = mixed[c].T
        for q in range(cols):
            block = times(mixed_t, xb[:, q * WIDE : (q + 1) * WIDE]).astype(BF16)
            act[2 * c : 2 * c + 2, :, :, 0:32, q * WIDE : (q + 1) * WIDE] = block.reshape(2, 2, 2, 32, WIDE)
    def mix_gradient():
        for copy in win_loads():
            copy.wait()

        def mix_part(block, q):
            span = slice(q * WIDE, (q + 1) * WIDE)
            return times_t(nf[rows_of(block), :], wg[span, 0:1024]) + times_t(nf[rows_of(2 + block), 0:512], wu[span, 0:512])

        for q in range(cols):
            m_mid(0, q).wait_send()
        for q in range(cols):
            sa[:, q * WIDE : (q + 1) * WIDE] = mix_part(1 - core, q).astype(BF16)
            m_mid(1, q).start()
        for q in range(cols):
            gno[:, q * WIDE : (q + 1) * WIDE] = mix_part(core, q)


    def final_output():
        m_out0.wait_recv()
        x_out.wait_recv()
        m_out0.wait_send()

        @pl.loop(0, half // 16, unroll=4)
        def _(r):
            at = pl.ds(pl.multiple_of(r * 16, 16), 16)
            outp[core, at, :] = (
                mid[at, :]
                + (outp[core, at, :].astype(F32) + outr[0, at, :].astype(F32) + outx[at, :].astype(F32))
            ).astype(BF16)


        m_final.start()
        out_copy.start()

    def input_gradient():
        for q in range(cols):
            m_mid(1, q).wait_recv()

        @pl.loop(0, half // 16, unroll=4)
        def _(r):
            at = pl.ds(pl.multiple_of(r * 16, 16), 16)
            grad = gno[at, :] + ra[at, :].astype(F32)
            stream = og[pl.ds(pl.multiple_of(rows + core * half + r * 16, 16), 16), :].astype(F32)
            scale = lax.rsqrt(mean_of(stream * stream) + EPSILON)
            weighted = grad * gain_mix[...].astype(F32)
            sums[0] += fold(grad * stream * scale)
            gm[at, :] += scale * weighted - stream * (scale * scale * scale) * mean_of(weighted * stream)

        m_in.start()
        in_copy.start()


    def gains_and_taps():
        lines = [jnp.sum(sums[0], axis=0, keepdims=True), jnp.sum(sums[1], axis=0, keepdims=True)]
        tap_lines = [[jnp.sum(taps_sum[c, k], axis=0, keepdims=True) for c in range(2)] for k in range(3)]
        for k in range(8):
            piece = [line[:, k * 128 : (k + 1) * 128] for line in lines]
            group = k // 2
            start = (group % 2) * 128
            piece += [tap_lines[t][group // 2][:, start : start + 128] for t in range(3)]
            tile = jnp.concatenate(piece + [jnp.zeros((3, 128), F32)], axis=0)
            for side in range(2):
                part_s[k // 2, k % 2, side] = tile

    m_final = send(13, outp.at[core], out_hbm.at[mine], mate)
    out_copy = load(8, outp.at[core], out_hbm.at[mine])
    in_copy = load(9, gm, in_grad_hbm.at[mine])

    stores = []

    def own_column(u):
        return pl.multiple_of(x * share + (u % groups) * GROUP, 128)

    def other_column(u):
        return pl.multiple_of((1 - x) * share + (u % groups) * GROUP, 128)

    def g_store(u, k):
        target = gate_hbm if u < groups else up_hbm
        column = own_column(u) if k == 0 else other_column(u)
        return pltpu.make_async_copy(stage_g.at[u, k], target.at[:, pl.ds(column, GROUP)], g_sem.at[u, k])

    def d_store(q):
        return pltpu.make_async_copy(stage_d.at[q], down_hbm.at[:, pl.ds(q * WIDE, WIDE)], d_sem.at[q])

    def i_store(i):
        return pltpu.make_async_copy(stage_i.at[i], in_hbm.at[i // 2, :, pl.ds((i % 2) * WIDE, WIDE)], m_sem.at[i])

    def o_store(q):
        return pltpu.make_async_copy(stage_o.at[q], outw_hbm.at[:, pl.ds(q * WIDE, WIDE)], m_sem.at[6 + q])

    def g3(u):
        stage_g[u, 0] = grads.run3(u)
        g_store(u, 0).start()

    def g4(u):
        stage_g[u, 1] = grads.run4(u)
        g_store(u, 1).start()

    def d6(q):
        downs.run6(q, stage_d.at[q])
        d_store(q).start()

    def i4(i):
        stage_i[i] = ins.run4(i, IN_FIRST[i])
        i_store(i).start()

    def o4(q):
        stage_o[q] = outs.run4(q, OUT_FIRST[q])
        o_store(q).start()

    def s4(u):
        stage_s[...] = smalls.run4(u, True)
        m_small.start()

    table = {
        "d1": downs.run1, "d2": downs.run2, "d3": downs.run3, "d4": downs.run4, "d5": lambda q: downs.run5(q, stage_d.at[q]), "d6": d6,
        "g1": grads.run1, "g2": grads.run2, "g3": g3, "g4": g4,
        "i1": lambda i: ins.run1(i, IN_FIRST[i]), "o1": lambda q: outs.run1(q, OUT_FIRST[q]), "s1": lambda u: smalls.run1(u, True),
        "i2": lambda i: ins.run2(i, IN_FIRST[i]), "i3": lambda i: ins.run3(i, IN_FIRST[i]), "i4": i4,
        "o2": lambda q: outs.run2(q, OUT_FIRST[q]), "o3": lambda q: outs.run3(q, OUT_FIRST[q]), "o4": o4,
        "s2": lambda u: smalls.run2(u, True), "s3": lambda u: smalls.run3(u, True), "s4": s4,
    }

    steps = {
        "Wt": [turn_activated],
        "Wd": [lambda q=q: down_part(q) for q in range(cols)],
        "Wg": [lambda: hidden_part(part_g, gg)],
        "Wu": [lambda: hidden_part(part_u, gu)],
        "gn0": [gradient_theirs],
        "gn1": [gradient_mine],
        "out": [output_both],
        "norm": [ffn_norm],
        "mixb": [mixer_back],
        "iA": [lambda i=i: in_grad_of(i) for i in (2, 3, 0, 4, 1, 5)],
        "hw": [lambda: gated_back(0)],
        "el": [lambda: gated_back(1)],
        "oA": [lambda c=c: out_grad_of(c) for c in range(2)],
        "gnm": [mix_gradient],
        "outf": [final_output],
        "ing": [input_gradient],
        "gain": [gains_and_taps],
    }
    for word in PROGRAM:
        if word in steps:
            steps[word].pop(0)()
        else:
            table[word[:2]](int(word[2:]))

    m_small.wait_recv()
    m_small.wait_send()
    keep = lax.broadcasted_iota(jnp.int32, (8, 128), 0) < 2
    stage_s[...] = stage_s[...] + jnp.where(keep, recv_s[...], 0.0)
    small_copy = load(10, stage_s, small_hbm)
    small_copy.start()

    for u in range(2 * groups):
        grads.drain(u)
        g_store(u, 0).wait()
        g_store(u, 1).wait()
    for q in range(cols):
        downs.drain(q)
        d_store(q).wait()
    for i in range(6):
        ins.drain(i, IN_FIRST[i])
        i_store(i).wait()
    for q in range(cols):
        outs.drain(q, OUT_FIRST[q])
        o_store(q).wait()
    smalls.drain(0, True)
    for copy in (small_copy, out_copy, in_copy):
        copy.wait()
    for copy in (x_og, m_gn0, m_gn1, x_gn, m_out1, x_out, m_rmid, m_in, m_final):
        copy.wait_send()
    m_in.wait_recv()
    m_final.wait_recv()
    for q in range(cols):
        m_mid(1, q).wait_send()
    for c in range(2):

        @pl.when(me < last)
        def _():
            halo_fwd(c).wait_send()

        @pl.when(me > 0)
        def _():
            halo_back(c).wait_send()


IN_FIRST = (True, True, True, True, True, True)
OUT_FIRST = (False, True, False, True)
PROGRAM = (
    "Wt", "Wd", "d10", "Wd", "Wd", "Wd", "Wg", "g12", "d11", "d20", "Wu", "d30", "g15", "gn0",
    "d12", "gn1", "d13", "g22", "out", "d21", "d31", "norm", "g25", "mixb", "d41", "iA", "i12", "iA",
    "d22", "g11", "hw", "g14", "iA", "g10", "d23", "d32", "d33", "iA", "i10", "el", "iA", "d42",
    "iA", "g21", "d43", "i14", "oA", "g13", "d40", "oA", "o13", "g24", "i13", "i22", "g20", "i15",
    "g31", "o11", "d52", "gnm", "i20", "i32", "g32", "g23", "i11", "o12", "d50", "i24", "i25", "i34",
    "o22", "o10", "o20", "outf", "i21", "i35", "d53", "o21", "d51", "g35", "i23", "ing", "o23", "g33",
    "i30", "o31", "i31", "g45", "gain", "g30", "s10", "o33", "g34", "o32", "i33", "o30", "i40", "d63",
    "g44", "g42", "i41", "i45", "o41", "d60", "d61", "i44", "g43", "s20", "s30", "o42", "g41", "i42",
    "g40", "d62", "o40", "i43", "o43", "s40",
)


def whole_block(inputs, out_grad, mix_gain, in_weight, conv_weight, out_weight, ffn_gain, gate_weight, up_weight, down_weight):
    rows, width = inputs.shape[1:]
    hidden = gate_weight.shape[2]
    channels = out_weight.shape[1]
    cols, share, half = width // WIDE, hidden // 2, rows // 2
    n = lax.axis_size("seq")

    def vm(*shape, kind=BF16):
        return pltpu.VMEM(shape, kind)

    def dma(*shape):
        return pltpu.SemaphoreType.DMA(shape)

    def buffers(count, length, lanes, kind):
        return [vm(count, 4, 2, length, lanes, kind=kind), vm(count, 4, length, lanes, kind=kind), vm(count, 3, length, lanes, kind=kind)]

    lq, ld, lo = width // n, hidden // n, channels // n
    hbm = pl.BlockSpec(memory_space=pl.ANY)
    vmem = pl.BlockSpec(memory_space=pltpu.VMEM)
    results = pl.pallas_call(
        block_kernel,
        out_shape=[
            jax.ShapeDtypeStruct((rows, width), BF16),
            jax.ShapeDtypeStruct((rows, width), F32),
            jax.ShapeDtypeStruct((lq, hidden), F32),
            jax.ShapeDtypeStruct((lq, hidden), F32),
            jax.ShapeDtypeStruct((ld, width), F32),
            jax.ShapeDtypeStruct((3, lq, channels), F32),
            jax.ShapeDtypeStruct((lo, width), F32),
            jax.ShapeDtypeStruct((8, 128), F32),
        ],
        in_specs=[hbm] * 7 + [vmem] * 3,
        out_specs=[hbm] * 8,
        scratch_shapes=[
            vm(rows, width), vm(2 * rows, width), vm(2 * rows, width), vm(width, 2 * rows),
            *[vm(4, 2, 2, 64, share)] * 3,
            *[vm(half, width, kind=F32)] * 3,
            vm(6, rows, WIDE, kind=F32), vm(2, rows + 8, WIDE, kind=F32), vm(2, rows + 8, WIDE, kind=F32),
            vm(2, rows, WIDE), vm(channels, width), vm(width, share), vm(width, share), vm(share, width),
            vm(3, half, share - 512, kind=F32),
            vm(half, width), vm(half, width),
            *[vm(4, half, width), vm(2, half, width), vm(half, width)] * 2,
            vm(2, 8, width, kind=F32), vm(2, 3, 8, WIDE, kind=F32),
            vm(4, 2, 2, lq, share), vm(4, 2, 2, lq, share),
            vm(6, 4, 2, lq, 384), vm(6, 3, 2, lq, 384), vm(6, lq, 384), vm(6, lq, 384),
            vm(cols, 2, 2, 2, ld, WIDE), vm(cols, 2, 2, ld, WIDE), vm(cols, 2, 2, ld, WIDE), vm(cols, 2, ld, WIDE),
            vm(cols, ld, WIDE), vm(cols, ld, WIDE),
            *buffers(6, lq, WIDE, BF16), *buffers(cols, lo, WIDE, BF16),
            vm(4, 2, 2, 8, 128, kind=F32), *buffers(1, 8, 128, F32), vm(8, 128, kind=F32),
            vm(6, 2, lq, 384, kind=F32), vm(cols, ld, WIDE, kind=F32), vm(6, lq, WIDE, kind=F32), vm(cols, lo, WIDE, kind=F32),
            vm(8, 128, kind=F32),
            dma(6), dma(6), dma(6, 3), dma(6, 3), dma(6), dma(6), *[dma(cols)] * 8,
            *[dma(11)] * 4, *[dma(11, 3)] * 2,
            dma(11), dma(15), dma(15), dma(2, cols), dma(2, cols), dma(4), dma(4), dma(6, 2), dma(cols), dma(10),
        ],
        compiler_params=pltpu.CompilerParams(collective_id=0, has_side_effects=True, vmem_limit_bytes=VMEM_BYTES),
    )(
        inputs[0], out_grad[0], in_weight.reshape(width, 3 * channels), out_weight[0],
        gate_weight[0], up_weight[0], down_weight[0], mix_gain, conv_weight[0], ffn_gain,
    )
    output, in_grad, gate_s, up_s, down_s, in_s, out_s, small = results
    index = lax.axis_index("seq")
    y, x = (index // 2) % 2, index % 2
    gains = lax.dynamic_slice(small, (0, x * 64), (2, 64))
    conv_s = lax.dynamic_slice(small, (2, y * 64 + x * 32), (3, 32))
    return (
        output[None], in_grad[None], gains[0:1], in_s.transpose(1, 0, 2)[None], conv_s[None],
        out_s[None], gains[1:2], gate_s[None], up_s[None], down_s[None],
    )


def inverse_rms(stream):
    return lax.rsqrt(jnp.mean(stream * stream, axis=-1, keepdims=True) + EPSILON)


def norm_back(grad_normed, stream, inv_scale, gain_vec):
    weighted = grad_normed * gain_vec
    gain_grad = jnp.sum(grad_normed * stream * inv_scale, axis=(0, 1))
    cubed = inv_scale * inv_scale * inv_scale
    grad_before = inv_scale * weighted - stream * cubed * jnp.mean(
        weighted * stream, axis=-1, keepdims=True
    )
    return (gain_grad, grad_before)


def forward_block(stream, weights):
    gain_mix, weight_in, weight_conv, weight_out, gain_ffn, weight_gate, weight_up, weight_down = (
        weights
    )
    seq_count, rows_in, model_width = stream.shape
    channels = weight_in.shape[-1]
    hidden = weight_gate.shape[-1]
    scale_mix = inverse_rms(stream)
    normed_mix = (stream * scale_mix * gain_mix.astype(jnp.float32)).astype(jnp.bfloat16)
    projected = jnp.dot(
        normed_mix.reshape(-1, model_width),
        weight_in.reshape(model_width, 3 * channels),
        preferred_element_type=jnp.float32,
    )
    projected = projected.reshape(seq_count, rows_in, 3, channels)
    gated_in = projected[:, :, 0] * projected[:, :, 2]
    carried = shifted(gated_in[:, -2:], "seq", 1)
    extended = jnp.concatenate([carried, gated_in], axis=1)
    out_rows = extended.shape[1] - 2
    kernel = weight_conv.astype(jnp.float32)
    convolved = (
        kernel[0] * extended[:, :out_rows]
        + kernel[1] * extended[:, 1 : out_rows + 1]
        + kernel[2] * extended[:, 2:]
    )
    mixed_out = (projected[:, -out_rows:, 1] * convolved).astype(jnp.bfloat16)
    partial_out = jnp.dot(
        mixed_out.reshape(-1, channels), weight_out, preferred_element_type=jnp.float32
    )
    middle = stream + pair_sum(partial_out).reshape(seq_count, out_rows, model_width)
    scale_ffn = inverse_rms(middle)
    normed_ffn = (middle * scale_ffn * gain_ffn.astype(jnp.float32)).astype(jnp.bfloat16)
    flat_ffn = normed_ffn.reshape(-1, model_width)
    gate_pre = jnp.dot(flat_ffn, weight_gate, preferred_element_type=jnp.float32)
    up_pre = jnp.dot(flat_ffn, weight_up, preferred_element_type=jnp.float32)
    activated = (jax.nn.silu(gate_pre) * up_pre).astype(jnp.bfloat16)
    partial_ffn = jnp.dot(activated, weight_down, preferred_element_type=jnp.float32)
    result = middle + pair_sum_low(partial_ffn).reshape(seq_count, out_rows, model_width)
    stored = (
        stream,
        scale_mix,
        normed_mix,
        projected,
        extended,
        convolved,
        mixed_out,
        middle,
        scale_ffn,
        normed_ffn,
        gate_pre.reshape(seq_count, out_rows, hidden),
        up_pre.reshape(seq_count, out_rows, hidden),
        activated.reshape(seq_count, out_rows, hidden),
    )
    return (result, stored)


def backward_ffn(grad_stream, stored, weights):
    gain_mix, weight_in, weight_conv, weight_out, gain_ffn, weight_gate, weight_up, weight_down = (
        weights
    )
    (
        block_in,
        scale_mix,
        normed_mix,
        projected,
        extended,
        convolved,
        mixed_out,
        middle,
        scale_ffn,
        normed_ffn,
        gate_pre,
        up_pre,
        activated,
    ) = stored
    seq_count, own_len, model_width = grad_stream.shape
    hidden = weight_gate.shape[-1]
    rounded = grad_stream.astype(jnp.bfloat16).reshape(-1, model_width)
    grad_hidden = jnp.einsum("nd,fd->nf", rounded, weight_down, preferred_element_type=jnp.float32)
    down_grad = jnp.einsum(
        "nf,nd->fd", activated.reshape(-1, hidden), rounded, preferred_element_type=jnp.float32
    )
    gate_flat = gate_pre.reshape(-1, hidden)
    up_flat = up_pre.reshape(-1, hidden)
    sigmoid_gate = jax.nn.sigmoid(gate_flat)
    grad_gate = (
        grad_hidden * up_flat * sigmoid_gate * (1.0 + gate_flat * (1.0 - sigmoid_gate))
    ).astype(jnp.bfloat16)
    grad_up = (grad_hidden * gate_flat * sigmoid_gate).astype(jnp.bfloat16)
    flat_ffn = normed_ffn.reshape(-1, model_width)
    gate_grad = jnp.einsum("nd,nf->df", flat_ffn, grad_gate, preferred_element_type=jnp.float32)
    up_grad = jnp.einsum("nd,nf->df", flat_ffn, grad_up, preferred_element_type=jnp.float32)
    partial_ffn = jnp.einsum(
        "nf,df->nd", grad_gate, weight_gate, preferred_element_type=jnp.float32
    )
    partial_ffn = partial_ffn + jnp.einsum(
        "nf,df->nd", grad_up, weight_up, preferred_element_type=jnp.float32
    )
    grad_normed = pair_sum(partial_ffn).reshape(seq_count, own_len, model_width)
    ffn_gain_grad, grad_middle = norm_back(
        grad_normed, middle, scale_ffn, gain_ffn.astype(jnp.float32)
    )
    grad_middle = grad_stream + grad_middle
    return (grad_middle, (ffn_gain_grad, gate_grad, up_grad, down_grad))


def backward_mixer(grad_middle, stored, weights):
    gain_mix, weight_in, weight_conv, weight_out, gain_ffn, weight_gate, weight_up, weight_down = (
        weights
    )
    (
        block_in,
        scale_mix,
        normed_mix,
        projected,
        extended,
        convolved,
        mixed_out,
        middle,
        scale_ffn,
        normed_ffn,
        gate_pre,
        up_pre,
        activated,
    ) = stored
    seq_count, own_len, model_width = grad_middle.shape
    channels = weight_out.shape[0]
    rounded_mid = grad_middle.astype(jnp.bfloat16).reshape(-1, model_width)
    grad_mixed = jnp.einsum(
        "nd,cd->nc", rounded_mid, weight_out, preferred_element_type=jnp.float32
    )
    grad_mixed = grad_mixed.reshape(seq_count, own_len, channels)
    out_grad_w = jnp.einsum(
        "nc,nd->cd",
        mixed_out.reshape(-1, channels),
        rounded_mid,
        preferred_element_type=jnp.float32,
    )
    grad_conv = grad_mixed * projected[:, :, 1]
    grad_second = grad_mixed * convolved
    following = shifted(grad_conv[:, :2], "seq", -1)
    ext_grad = jnp.concatenate([grad_conv, following], axis=1)
    kernel = weight_conv.astype(jnp.float32)
    grad_gated = (
        kernel[0] * ext_grad[:, 2:] + kernel[1] * ext_grad[:, 1:-1] + kernel[2] * ext_grad[:, :-2]
    )
    conv_grad = jnp.stack(
        [
            jnp.sum(grad_conv * extended[:, offset : offset + own_len], axis=(0, 1))
            for offset in range(3)
        ]
    )
    grad_proj = jnp.stack(
        [grad_gated * projected[:, :, 2], grad_second, grad_gated * projected[:, :, 0]], axis=2
    )
    grad_proj = grad_proj.astype(jnp.bfloat16).reshape(-1, 3 * channels)
    in_grad_w = jnp.einsum(
        "nd,nk->dk",
        normed_mix.reshape(-1, model_width),
        grad_proj,
        preferred_element_type=jnp.float32,
    )
    in_grad_w = in_grad_w.reshape(model_width, 3, channels)
    partial_mix = jnp.einsum(
        "nk,dk->nd",
        grad_proj,
        weight_in.reshape(model_width, 3 * channels),
        preferred_element_type=jnp.float32,
    )
    grad_normed_mix = (
        pair_sum_low(partial_mix)
        .reshape(seq_count, own_len, model_width)
    )
    mix_gain_grad, grad_input = norm_back(
        grad_normed_mix, block_in, scale_mix, gain_mix.astype(jnp.float32)
    )
    grad_input = grad_middle + grad_input
    return (grad_input, (mix_gain_grad, in_grad_w, conv_grad, out_grad_w))


def local(
    inputs,
    out_grad,
    mix_gain,
    in_weight,
    conv_weight,
    out_weight,
    ffn_gain,
    gate_weight,
    up_weight,
    down_weight,
):
    if lax.axis_size("seq") == 16:
        return whole_block(
            inputs, out_grad, mix_gain, in_weight, conv_weight, out_weight, ffn_gain, gate_weight, up_weight, down_weight
        )
    layer_count = mix_gain.shape[0]

    def weights_of(number):
        return (
            mix_gain[number],
            in_weight[number],
            conv_weight[number],
            out_weight[number],
            ffn_gain[number],
            gate_weight[number],
            up_weight[number],
            down_weight[number],
        )

    stream = inputs.astype(jnp.float32)
    number = 0
    stream, stored = forward_block(stream, weights_of(number))
    stored_all = [stored]
    output = stream.astype(jnp.bfloat16)
    grad_stream = out_grad.astype(jnp.float32)
    ffn_parts = [None] * layer_count
    mixer_parts = [None] * layer_count
    for number in reversed(range(layer_count)):
        grad_middle, ffn_terms = backward_ffn(grad_stream, stored_all[number], weights_of(number))
        ffn_parts[number] = ffn_terms
        grad_stream, mixer_terms = backward_mixer(
            grad_middle, stored_all[number], weights_of(number)
        )
        mixer_parts[number] = mixer_terms
    joined = tuple(mixer_parts[0]) + tuple(ffn_parts[0])
    mix_gain_g, in_g, conv_g, out_g, ffn_gain_g, gate_g, up_g, down_g = joined
    n = lax.axis_size("seq")
    down_s = scatter_sum(down_g.astype(jnp.bfloat16), (0, 1, 2))
    gate_s = scatter_sum(gate_g.astype(jnp.bfloat16), (2, 1, 0))
    up_s = scatter_sum(up_g.astype(jnp.bfloat16), (1, 2, 0))
    out_s = scatter_sum(out_g.astype(jnp.bfloat16), (1, 2, 0))
    in_s = scatter_sum(in_g.astype(jnp.bfloat16), (2, 1, 0))
    taps, channels = conv_g.shape
    small = jnp.concatenate(
        [
            mix_gain_g.reshape(n, -1),
            ffn_gain_g.reshape(n, -1),
            conv_g.reshape(taps, n, -1).swapaxes(0, 1).reshape(n, -1),
        ],
        axis=1,
    )
    small = scatter_sum(small, (2, 1, 0), jnp.float32).reshape(-1)
    gain_len = mix_gain_g.shape[0] // n
    return (
        output,
        grad_stream,
        small[:gain_len][None],
        in_s[None],
        small[2 * gain_len :].reshape(1, taps, channels // n),
        out_s[None],
        small[gain_len : 2 * gain_len][None],
        gate_s[None],
        up_s[None],
        down_s[None],
    )


def solution(mesh):
    in_specs = (
        P(None, "seq", None),
        P(None, "seq", None),
        P(),
        P(None, None, None, "tensor"),
        P(None, None, "tensor"),
        P(None, "tensor", None),
        P(),
        P(None, None, "tensor"),
        P(None, None, "tensor"),
        P(None, "tensor", None),
    )
    out_specs = (
        P(None, "seq", None),
        P(None, "seq", None),
        P(None, "seq"),
        P(None, "seq", None, "tensor"),
        P(None, None, ("tensor", "seq")),
        P(None, ("tensor", "seq"), None),
        P(None, "seq"),
        P(None, "seq", "tensor"),
        P(None, "seq", "tensor"),
        P(None, ("tensor", "seq"), None),
    )
    return jax.shard_map(local, mesh=mesh, in_specs=in_specs, out_specs=out_specs, check_vma=False)
```
